32 devices in a mesh: row: 8 (over z, y), col: 4 (over x, core).
Axes of the slice: x: 2, y: 2, z: 4, core: 2. Of those that a mesh axis runs over, the one named last changes fastest.
Arguments:
- layer_input: bfloat16 [2048, 8192], P('row'), may hold values from -7 to 7
- gain: float32 [8192], replicated, may hold values from 0.5 to 6
- d_query: bfloat16 [2048, 4096], P('row', 'col'), may hold values from -6 to 6
- d_keyval: bfloat16 [2048, 2048], P('row', 'col'), may hold values from -6 to 6
- w_query: bfloat16 [8192, 4096], P('row', 'col'), may hold values from -0.0625 to 0.0625
- w_keyval: bfloat16 [8192, 2048], P('row', 'col'), may hold values from -1 to 1
- d_resid: bfloat16 [2048, 8192], P('row', 'col'), may hold values from -6 to 6
Outputs:
- d_input: bfloat16 [2048, 8192], P('row', 'col')
- grad_wq: bfloat16 [8192, 4096], P('row', 'col')
- grad_wkv: bfloat16 [8192, 2048], P('row', 'col')
- grad_gain: float32 [8192], P('col')
- grad_square_sum: float32 [], replicated
The draws below stay inside these ranges and needn't reach their ends.
All inputs are finite; a program needn't handle non-finite values.
Results may differ from the reference program's by a relative error of at most 0.023.
Values may be sent and summed in bfloat16 or wider, within the bound.
A program may use at most 128 MiB of HBM per device.

```python
import jax
import jax.numpy as jnp
from jax import lax

D = 8192
TOK_DEV = 256
QW = 4096
KVW = 2048
TOKENS = 2048
N_ROW = 8
N_COL = 4


def input_values(key):
    input_key = jax.random.fold_in(key, 101)
    return jnp.clip(jax.random.normal(input_key, (TOKENS, D), jnp.float32), -6.0, 6.0)


def keyval_values(key):
    weight_key = jax.random.fold_in(key, 202)
    factor = jnp.float32(1.0) / jnp.sqrt(jnp.float32(D))
    return jnp.clip(jax.random.normal(weight_key, (D, KVW), jnp.float32), -6.0, 6.0) * factor


def draw_layer_input(key, part):
    return input_values(key).astype(jnp.bfloat16)


def draw_gain(key, part):
    gain_key = jax.random.fold_in(key, 404)
    position = jnp.arange(D, dtype=jnp.float32) / jnp.float32(max(D - 1, 1))
    ramp = 1.0 + 2.0 * position
    factor = jax.random.uniform(gain_key, (D,), jnp.float32, 0.85, 1.15)
    return ramp * factor


def draw_w_keyval(key, part):
    return keyval_values(key).astype(jnp.bfloat16)


def draw_d_keyval(key, part):
    inputs = input_values(key)
    weights = keyval_values(key)
    scaled = inputs * lax.rsqrt(jnp.mean(inputs * inputs, axis=1, keepdims=True) + 1e-05)
    projected = jnp.dot(scaled, weights, precision=lax.Precision.HIGHEST)
    noise_key = jax.random.fold_in(key, 303)
    noise = jax.random.normal(noise_key, (TOKENS, KVW), jnp.float32)
    return jnp.clip(0.6 * projected + 0.8 * noise, -6.0, 6.0).astype(jnp.bfloat16)


def levels(own_key, shape, cuts, smallest, largest):
    def one(axis_at, blocks):
        heights = jax.random.uniform(jax.random.fold_in(jax.random.fold_in(own_key, 6), axis_at), (blocks,), jnp.float32, smallest / len(cuts), largest / len(cuts))
        return jnp.repeat(jnp.exp(heights), shape[axis_at] // blocks).reshape((-1,) + (1,) * (len(shape) - axis_at - 1))

    loudness = one(*cuts[0])
    for cut in cuts[1:]:
        loudness = loudness * one(*cut)
    return loudness


def bell_draw(rng, extent, deviation, bound, cuts=(), kind=jnp.bfloat16):
    entries = jax.random.normal(rng, extent, jnp.float32) * deviation
    if len(cuts) > 0:
        entries = levels(rng, extent, cuts, -0.22, 0.18) * entries
    return jnp.clip(entries, min=-bound, max=bound).astype(kind)


def setup_inputs(seed: int = 0) -> dict:
    arg_keys = jax.random.split(jax.random.key(seed), 8)
    layer_input = draw_layer_input(jax.random.fold_in(arg_keys[7], 71), 0)
    gain = draw_gain(jax.random.fold_in(arg_keys[7], 71), 0)
    d_query = bell_draw(arg_keys[2], (TOKENS, QW), 1.0, 6.0, ((0, 8), (1, 4)))
    d_keyval = draw_d_keyval(jax.random.fold_in(arg_keys[7], 71), 0)
    w_query = bell_draw(arg_keys[4], (D, QW), D ** -0.5, 0.0625, ((0, 8), (1, 4)))
    w_keyval = draw_w_keyval(jax.random.fold_in(arg_keys[7], 71), 0)
    d_resid = bell_draw(arg_keys[6], (TOKENS, D), 1.0, 6.0, ((0, 8), (1, 4)))
    return dict(layer_input=layer_input, gain=gain, d_query=d_query, d_keyval=d_keyval, w_query=w_query, w_keyval=w_keyval, d_resid=d_resid)


epsilon = 1e-05

def reference(layer_input, gain, d_query, d_keyval, w_query, w_keyval, d_resid):
    inputs = layer_input.astype(jnp.float32)
    inv_rms = lax.rsqrt(lax.optimization_barrier(jnp.mean(inputs * inputs, axis=1, keepdims=True)) + epsilon)
    normed = (inputs * inv_rms * gain).astype(jnp.bfloat16)
    query_cols = QW // N_COL
    keyval_cols = KVW // N_COL
    contract_cols = (((1,), (1,)), ((), ()))

    def add_block(block, accum_grad):
        qstart = (block * query_cols).astype(jnp.int32)
        kstart = (block * keyval_cols).astype(jnp.int32)
        qgrad = lax.dynamic_slice_in_dim(d_query, qstart, query_cols, 1)
        qweight = lax.dynamic_slice_in_dim(w_query, qstart, query_cols, 1)
        kgrad = lax.dynamic_slice_in_dim(d_keyval, kstart, keyval_cols, 1)
        kweight = lax.dynamic_slice_in_dim(w_keyval, kstart, keyval_cols, 1)
        partial_value = lax.dot_general(qgrad, qweight, contract_cols, preferred_element_type=jnp.float32)
        partial_value = partial_value + lax.dot_general(kgrad, kweight, contract_cols, preferred_element_type=jnp.float32)
        return accum_grad + partial_value.astype(jnp.bfloat16).astype(jnp.float32)
    feature_grad = lax.fori_loop(0, N_COL, add_block, jnp.zeros((TOKENS, D), jnp.float32))
    token_dot = lax.optimization_barrier(jnp.sum(gain * feature_grad * inputs, axis=1, keepdims=True))
    d_input = (d_resid.astype(jnp.float32) + inv_rms * gain * feature_grad - inputs * inv_rms ** 3 * token_dot / D).astype(jnp.bfloat16)
    scaling = 1.0 / jnp.sqrt(jnp.float32(TOKENS))
    grad_gain = lax.optimization_barrier(jnp.sum(feature_grad * inputs * inv_rms, axis=0)) * scaling
    weight_scale = 1.0 / jnp.sqrt(jnp.float32(TOK_DEV))
    contract_rows = (((0,), (0,)), ((), ()))

    def add_tokens(block, accums):
        tstart = (block * TOK_DEV).astype(jnp.int32)
        slab = lax.dynamic_slice_in_dim(normed, tstart, TOK_DEV, 0)
        qgrad = lax.dynamic_slice_in_dim(d_query, tstart, TOK_DEV, 0)
        kgrad = lax.dynamic_slice_in_dim(d_keyval, tstart, TOK_DEV, 0)
        block_q = lax.dot_general(slab, qgrad, contract_rows, preferred_element_type=jnp.float32) * weight_scale
        block_kv = lax.dot_general(slab, kgrad, contract_rows, preferred_element_type=jnp.float32) * weight_scale
        return (accums[0] + block_q.astype(jnp.bfloat16).astype(jnp.float32), accums[1] + block_kv.astype(jnp.bfloat16).astype(jnp.float32))
    sum_q, sum_kv = lax.fori_loop(0, N_ROW, add_tokens, (jnp.zeros((D, QW), jnp.float32), jnp.zeros((D, KVW), jnp.float32)))
    grad_wq = sum_q.astype(jnp.bfloat16)
    grad_wkv = sum_kv.astype(jnp.bfloat16)
    query_f = grad_wq.astype(jnp.float32)
    keyval_f = grad_wkv.astype(jnp.float32)
    grand_total = jnp.sum(query_f * query_f) + jnp.sum(keyval_f * keyval_f) + jnp.sum(grad_gain * grad_gain)
    grad_square_sum = grand_total / jnp.float32(D)
    return (d_input, grad_wq, grad_wkv, grad_gain, grad_square_sum)
```

```python
import functools
import math

import jax
import jax.numpy as jnp
from jax import lax
from jax.experimental import pallas as pl
from jax.experimental.pallas import tpu as pltpu
from jax.sharding import PartitionSpec as P

epsilon = 1e-05
MESH = pl.DeviceIdType.MESH
F32 = jnp.float32
BF16 = jnp.bfloat16
SWAPS = 4


def tile(size, limit):
    return limit if size % limit == 0 else size


def step_kernel(
    n_row, n_col,
    x_hbm, gain, dq_hbm, dk_hbm, wq_hbm, wk_hbm, resid_hbm,
    dinput_hbm, gwq_hbm, gwk_hbm, gains_out, total_out,
    cotq, cotk, xin, normed, ncols, wq, wk, resid, pfull, precv, csend, xrecv, fg,
    gq, gk, dout, inv, sq, dots, dots_in, gains, gains_in, tot, tot_in,
    load_sem, cot_send, cot_recv, swap_send, swap_recv, xs_send, xs_recv,
    cs_send, cs_recv, pe_send, pe_recv, xr_send, xr_recv, fs_send, fs_recv,
    out_sem, dot_send, dot_recv, gain_send, gain_recv, tot_send, tot_recv,
):
    row, col = lax.axis_index("row"), lax.axis_index("col")
    tokens, width = xin.shape
    half = tokens // 2
    part = tokens // n_col
    feats = width // n_row
    slice_width = width // n_col
    fold = n_row // n_col
    n_o, n_x = n_row // 2, n_col // 2
    o, y = row // 2, row % 2
    x, core = col // 2, col % 2
    mate = row + 1 - 2 * y
    home_col = row // fold
    home_x = home_col // 2
    at_home = x == home_x

    def remote(src, dst, send, recv, to_row, to_col):
        return pltpu.make_async_remote_copy(
            src_ref=src, dst_ref=dst, send_sem=send, recv_sem=recv,
            device_id=(to_row, to_col), device_id_type=MESH,
        )

    barrier = pltpu.get_barrier_semaphore()

    def greet_plane(k, carry):
        r = (row + k // 2) % n_row
        c = 2 * x + (core + k % 2) % 2
        pl.semaphore_signal(barrier, inc=1, device_id=(r, c), device_id_type=MESH)
        return carry

    lax.fori_loop(1, 2 * n_row, greet_plane, 0)

    def greet_cols(k, carry):
        c = (2 * x + k) % n_col
        pl.semaphore_signal(barrier, inc=1, device_id=(row, c), device_id_type=MESH)
        return carry

    lax.fori_loop(2, n_col, greet_cols, 0)
    x_copy = pltpu.make_async_copy(x_hbm, xin, load_sem.at[0])
    x_copy.start()
    pl.semaphore_wait(barrier, 2 * n_row - 1 + n_col - 2)

    def block(i):
        return pl.ds(pl.multiple_of(i * tokens, tokens), tokens)

    def nth(j):
        m = jnp.where(o < n_o - 1 - o, o, n_o - 1 - o)
        d = jnp.where(j <= 2 * m, (j + 1) // 2, j - m)
        up = jnp.where(j <= 2 * m, j % 2 == 0, o < n_o - 1 - o)
        return jnp.where(up, o + d, o - d)

    pieces = ((dq_hbm, cotq), (dk_hbm, cotk))

    def cot_copy(j, way, p, source, to_row, own):
        held = pieces[p][1].at[block(source)]
        return remote(
            pieces[p][0] if own else held, held,
            cot_send.at[j, way, p], cot_recv.at[source, p], to_row, col,
        )

    for p in range(2):
        cot_copy(0, 2, p, row, mate, True).start()

        @pl.when(o + 1 < n_o)
        def _():
            cot_copy(0, 0, p, row, row + 2, True).start()

        @pl.when(o > 0)
        def _():
            cot_copy(0, 1, p, row, row - 2, True).start()

    keep = [
        pltpu.make_async_copy(dq_hbm, cotq.at[block(row)], load_sem.at[1]),
        pltpu.make_async_copy(dk_hbm, cotk.at[block(row)], load_sem.at[2]),
        pltpu.make_async_copy(wq_hbm, wq, load_sem.at[3]),
        pltpu.make_async_copy(wk_hbm, wk, load_sem.at[4]),
    ]
    late = pltpu.make_async_copy(resid_hbm, resid, load_sem.at[5])
    x_copy.wait()
    for copy in keep:
        copy.start()
    late.start()

    rows_step = 16

    def norm_rows(i, carry):
        rows = pl.ds(pl.multiple_of(i * rows_step, rows_step), rows_step)
        values = xin[rows, :].astype(F32)
        mean = jnp.sum(values * values, axis=1, keepdims=True) / width
        scale = lax.rsqrt(mean + epsilon)
        inv[rows, :] = jnp.broadcast_to(scale, (rows_step, 128))
        normed[rows, :] = (values * scale * gain[...]).astype(BF16)
        return carry

    lax.fori_loop(0, tokens // rows_step, norm_rows, 0)
    own_cols = pl.ds(pl.multiple_of(row * feats, feats), feats)
    ncols[block(row), :] = normed[:, own_cols]
    for copy in keep:
        copy.wait()

    def quarter(source, c):
        start = pl.multiple_of(source * tokens + c * part, part)
        return ncols.at[pl.ds(start, part)]

    def swap_copy(k):
        target = (row + k) % n_row
        src = normed.at[
            pl.ds(pl.multiple_of(col * part, part), part),
            pl.ds(pl.multiple_of(target * feats, feats), feats),
        ]
        return remote(
            src, quarter(row, col), swap_send.at[k], swap_recv.at[row], target, col
        )

    def swap_arrival(source):
        return remote(
            quarter(source, col), quarter(source, col),
            swap_send.at[0], swap_recv.at[source], row, 2 * x + 1 - core,
        )

    def x_share(source, i):
        to_x = (x + i) % n_x
        return remote(
            quarter(source, col), quarter(source, col),
            xs_send.at[source, i], xs_recv.at[source, x], row, 2 * to_x + core,
        )

    def x_arrival(source, i):
        c = 2 * ((x + n_x - i) % n_x) + core
        return remote(
            quarter(source, c), quarter(source, c),
            xs_send.at[source, i], xs_recv.at[source, (x + n_x - i) % n_x],
            row, 2 * x + 1 - core,
        )

    def core_share(source, from_x, c):
        return remote(
            quarter(source, c), quarter(source, c),
            cs_send.at[source, from_x], cs_recv.at[source, from_x],
            row, 2 * x + 1 - core,
        )

    def swap_step(j, base, action):
        def one(i, carry):
            k = SWAPS * (j - base) + i + 1

            @pl.when((k >= 1) & (k < n_row))
            def _():
                action(k)

            return carry

        lax.fori_loop(0, SWAPS, one, 0)

    def share_first(k):
        source = (row + n_row - k) % n_row
        swap_arrival(source).wait_recv()
        for i in range(1, n_x):
            x_share(source, i).start()
        core_share(source, x, col).start()

    def share_second(k):
        source = (row + n_row - k) % n_row
        for i in range(1, n_x):
            x_arrival(source, i).wait_recv()
            from_x = (x + n_x - i) % n_x
            core_share(source, from_x, 2 * from_x + core).start()

    contract = (((1,), (1,)), ((), ()))
    f_tile = tile(feats, 256)
    own_half = pl.multiple_of(core * half, half)
    other_half = pl.multiple_of((1 - core) * half, half)

    def half_rows(source, start):
        return pl.ds(pl.multiple_of(source * tokens + start, half), half)

    def slot(source):
        return pl.ds(pl.multiple_of(source * half, half), half)

    def pair_copy(source):
        return remote(
            pfull.at[half_rows(source, other_half)], precv.at[slot(source)],
            pe_send.at[source], pe_recv.at[source], row, 2 * x + 1 - core,
        )

    def cross_copy(source):
        return remote(
            csend.at[slot(source)], xrecv.at[x, slot(source)],
            xr_send.at[source], xr_recv.at[x, source], row, 2 * home_x + core,
        )

    def home_copy(source):
        return remote(
            csend.at[slot(source)], fg.at[row % fold, pl.ds(own_half, half)],
            fs_send.at[source], fs_recv.at[row % fold, core], source, home_col,
        )

    def stage_one(source):
        def one(i, carry):
            fs = pl.ds(pl.multiple_of(i * f_tile, f_tile), f_tile)
            value = lax.dot_general(
                cotq[block(source), :], wq[fs, :], contract, preferred_element_type=F32
            ) + lax.dot_general(
                cotk[block(source), :], wk[fs, :], contract, preferred_element_type=F32
            )
            pfull[block(source), fs] = value.astype(BF16)
            return carry

        lax.fori_loop(0, feats // f_tile, one, 0)
        pair_copy(source).start()

    add_rows = tile(half, 32)

    def stage_two(source):
        pair_copy(source).wait_recv()

        @pl.when(jnp.logical_not(at_home))
        def _():
            def one(i, carry):
                at = i * add_rows
                mine = pl.ds(pl.multiple_of(source * tokens + own_half + at, add_rows), add_rows)
                rows = pl.ds(pl.multiple_of(source * half + at, add_rows), add_rows)
                value = pfull[mine, :].astype(F32) + precv[rows, :].astype(F32)
                csend[rows, :] = value.astype(BF16)
                return carry

            lax.fori_loop(0, half // add_rows, one, 0)
            cross_copy(source).start()

    def stage_three(source):
        @pl.when(at_home)
        def _():
            for i in range(1, n_x):
                from_x = (x + i) % n_x
                remote(
                    csend.at[slot(source)], xrecv.at[from_x, slot(source)],
                    xr_send.at[source], xr_recv.at[from_x, source],
                    row, 2 * x + 1 - core,
                ).wait_recv()

            def one(i, carry):
                at = i * add_rows
                mine = pl.ds(pl.multiple_of(source * tokens + own_half + at, add_rows), add_rows)
                rows = pl.ds(pl.multiple_of(source * half + at, add_rows), add_rows)
                value = pfull[mine, :].astype(F32) + precv[rows, :].astype(F32)
                for k in range(1, n_x):
                    value = value + xrecv[(x + k) % n_x, rows, :].astype(F32)
                csend[rows, :] = value.astype(BF16)
                return carry

            lax.fori_loop(0, half // add_rows, one, 0)
            here = (source == row) & (home_col == col)

            @pl.when(jnp.logical_not(here))
            def _():
                home_copy(source).start()

            @pl.when(here)
            def _():
                fg[row % fold, pl.ds(own_half, half), :] = csend[slot(source), :]

    down = (((0,), (0,)), ((), ()))
    weight_scale = 1.0 / math.sqrt(tokens)
    groups = []
    for held, kept, out in ((cotq, gq, gwq_hbm), (cotk, gk, gwk_hbm)):
        groups.append((held, kept, out, tile(held.shape[1], 512)))

    def out_copy(g, fs, i):
        _, kept, out, _ = groups[g]
        return pltpu.make_async_copy(kept.at[fs], out.at[fs], out_sem.at[g, i])

    def weight_tile(i, carry):
        fs = pl.ds(pl.multiple_of(i * f_tile, f_tile), f_tile)
        for g, (held, kept, _, k_tile) in enumerate(groups):
            for k in range(held.shape[1] // k_tile):
                ks = pl.ds(k * k_tile, k_tile)
                value = lax.dot_general(
                    ncols[:, fs], held[:, ks], down, preferred_element_type=F32
                )
                value = (value * weight_scale).astype(BF16)
                kept[fs, ks] = value
                value = value.astype(F32)
                value = jnp.sum(value * value, axis=0, keepdims=True)
                for part_at in range(k_tile // 128):
                    sq[...] += value[:, part_at * 128 : (part_at + 1) * 128]
            out_copy(g, fs, i).start()
        return carry

    f_tiles = feats // f_tile
    early_tiles = f_tiles // 2
    sq[...] = jnp.zeros_like(sq)

    def main_step(j, carry):
        @pl.when((j >= 1) & (j < n_o))
        def _():
            line = nth(j)
            source = 2 * line + y
            rising = line < o
            onward = jnp.where(rising, o + 1 < n_o, o > 0)
            to_row = jnp.where(rising, row + 2, row - 2)
            for p in range(2):
                cot_copy(j, 0, p, source, mate, False).wait_recv()

                @pl.when(onward)
                def _():
                    cot_copy(j, 0, p, source, to_row, False).start()

                cot_copy(j, 2, p, source, mate, False).start()

        swap_step(j, 0, lambda k: swap_copy(k).start())
        swap_step(j, 2, share_first)
        swap_step(j, 3, share_second)

        def source_of(b):
            return 2 * nth(j - b) + jnp.where(b == 0, y, 1 - y)

        def each(action):
            def one(b, carry):
                @pl.when(jnp.where(b == 0, j < n_o, j >= 1))
                def _():
                    action(source_of(b), b)

                return carry

            lax.fori_loop(0, 2, one, 0)

        def first(source, b):
            @pl.when(b == 1)
            def _():
                for p in range(2):
                    cot_copy(0, 0, p, source, mate, False).wait_recv()

            stage_one(source)

        each(first)
        each(lambda source, b: stage_two(source))

        @pl.when(j == n_o)
        def _():
            def wait_one(k, carry):
                source = (row + k) % n_row
                for from_x in range(n_x):
                    core_share(source, from_x, 2 * from_x + 1 - core).wait_recv()
                return carry

            lax.fori_loop(1, n_row, wait_one, 0)
            lax.fori_loop(0, early_tiles, weight_tile, 0)

        each(lambda source, b: stage_three(source))
        return carry

    lax.fori_loop(0, n_o + 1, main_step, 0)
    lax.fori_loop(early_tiles, f_tiles, weight_tile, 0)

    for j in range(fold):
        for c in range(2):
            @pl.when(jnp.logical_not((col * fold + j == row) & (c == core)))
            def _():
                arrived = fg.at[j, pl.ds(c * half, half)]
                remote(
                    arrived, arrived, fs_send.at[0], fs_recv.at[j, c], row, 2 * x + 1 - core
                ).wait_recv()

    late.wait()
    col_start = col * slice_width
    c_tile = tile(feats, 256)
    model_width = width
    tiles = feats // c_tile

    def lanes(value):
        total = value[:, 0:128]
        for k in range(1, c_tile // 128):
            total = total + value[:, k * 128 : (k + 1) * 128]
        return total

    def wide(value):
        return jnp.concatenate([value] * (c_tile // 128), axis=1)

    acc = jnp.zeros((tokens, 128), F32)
    for j in range(fold):
        for t in range(tiles):
            at = j * feats + t * c_tile
            here = pl.ds(pl.multiple_of(col_start + at, 128), c_tile)
            product = fg[j, :, t * c_tile : (t + 1) * c_tile].astype(F32) * xin[:, here].astype(F32)
            acc = acc + lanes(product * gain[:, here])
            gains[:, at : at + c_tile] = jnp.sum(product * wide(inv[...]), axis=0, keepdims=True)
    summed = jnp.broadcast_to(jnp.sum(acc, axis=1, keepdims=True), (tokens, 128))
    dots[...] = jnp.transpose(summed)[0:8, :]
    gains[:, slice_width:] = sq[...]

    dot_copies, gain_copies = [], []
    for k in range(1, n_col):
        dot_copies.append(
            remote(dots, dots_in.at[col], dot_send.at[k], dot_recv.at[k], row, (col + k) % n_col)
        )
    for k in range(1, n_row):
        gain_copies.append(
            remote(gains, gains_in.at[row], gain_send.at[k], gain_recv.at[k], (row + k) % n_row, col)
        )
    for copy in dot_copies + gain_copies:
        copy.start()
    dots_in[col] = dots[...]
    gains_in[row] = gains[...]
    for copy in gain_copies:
        copy.wait()
    all_gains = jnp.sum(gains_in[...], axis=0)
    grad_gain = all_gains[:, :slice_width] * (1.0 / math.sqrt(tokens * n_row))
    gains_out[...] = grad_gain
    squares = jnp.sum(grad_gain * grad_gain) + jnp.sum(all_gains[:, slice_width:])
    tot[...] = jnp.full(tot.shape, squares, F32)
    tot_copies = [
        remote(tot, tot_in.at[col], tot_send.at[k], tot_recv.at[k], row, (col + k) % n_col)
        for k in range(1, n_col)
    ]
    for copy in tot_copies:
        copy.start()
    tot_in[col] = tot[...]
    for copy in dot_copies:
        copy.wait()
    token_row = jnp.sum(dots_in[...], axis=0)[0:1, :]
    token_dot = jnp.transpose(jnp.broadcast_to(token_row, (128, tokens)))
    inv_rms = inv[...]
    inv_wide = wide(inv_rms)
    factor = wide(inv_rms * inv_rms * inv_rms * token_dot / model_width)
    d_copies = []
    for j in range(fold):
        for t in range(tiles):
            at = j * feats + t * c_tile
            here = pl.ds(pl.multiple_of(col_start + at, 128), c_tile)
            grad = fg[j, :, t * c_tile : (t + 1) * c_tile].astype(F32)
            value = (
                resid[:, at : at + c_tile].astype(F32)
                + inv_wide * gain[:, here] * grad
                - xin[:, here].astype(F32) * factor
            )
            dout[:, at : at + c_tile] = value.astype(BF16)
        span = pl.ds(j * feats, feats)
        copy = pltpu.make_async_copy(dout.at[:, span], dinput_hbm.at[:, span], load_sem.at[6 + j])
        copy.start()
        d_copies.append(copy)
    for copy in tot_copies:
        copy.wait()
    total_out[...] = jnp.sum(tot_in[...], axis=0) / model_width

    for copy in d_copies:
        copy.wait()
    for g in range(2):
        for i in range(f_tiles):
            out_copy(g, pl.ds(i * f_tile, f_tile), i).wait()
    for p in range(2):
        cot_copy(0, 2, p, row, mate, True).wait_send()

        @pl.when(o + 1 < n_o)
        def _():
            cot_copy(0, 0, p, row, row + 2, True).wait_send()

        @pl.when(o > 0)
        def _():
            cot_copy(0, 1, p, row, row - 2, True).wait_send()

    def drain_line(j, carry):
        line = nth(j)
        onward = jnp.where(line < o, o + 1 < n_o, o > 0)
        for p in range(2):
            cot_copy(j, 2, p, 2 * line + y, mate, False).wait_send()

            @pl.when(onward)
            def _():
                cot_copy(j, 0, p, 2 * line + y, mate, False).wait_send()

        return carry

    lax.fori_loop(1, n_o, drain_line, 0)

    def drain_row(k, carry):
        source = (row + k) % n_row
        pair_copy(source).wait_send()

        @pl.when(jnp.logical_not(at_home))
        def _():
            cross_copy(source).wait_send()

        @pl.when(at_home & jnp.logical_not((source == row) & (home_col == col)))
        def _():
            home_copy(source).wait_send()

        @pl.when(k >= 1)
        def _():
            swap_copy(k).wait_send()
            for i in range(1, n_x):
                x_share(source, i).wait_send()
            for from_x in range(n_x):
                core_share(source, from_x, col).wait_send()

        return carry

    lax.fori_loop(0, n_row, drain_row, 0)


def local(layer_input, gain, d_query, d_keyval, w_query, w_keyval, d_resid):
    n_row, n_col = lax.axis_size("row"), lax.axis_size("col")
    n_x, n_o, fold = n_col // 2, n_row // 2, n_row // n_col
    tokens, width = layer_input.shape
    q_cols, k_cols = d_query.shape[1], d_keyval.shape[1]
    feats, slice_width = width // n_row, width // n_col
    half = tokens // 2
    f_tiles = feats // tile(feats, 256)
    dma = pltpu.SemaphoreType.DMA
    hbm = pl.BlockSpec(memory_space=pl.ANY)
    vmem = pl.BlockSpec(memory_space=pltpu.VMEM)
    shape = jax.ShapeDtypeStruct
    every = n_row * tokens
    d_input, grad_wq, grad_wkv, grad_gain, total = pl.pallas_call(
        functools.partial(step_kernel, n_row, n_col),
        out_shape=(
            shape((tokens, slice_width), BF16),
            shape((feats, q_cols), BF16),
            shape((feats, k_cols), BF16),
            shape((1, slice_width), F32),
            shape((1, 128), F32),
        ),
        in_specs=[hbm, vmem, hbm, hbm, hbm, hbm, hbm],
        out_specs=[hbm, hbm, hbm, vmem, vmem],
        scratch_shapes=[
            pltpu.VMEM((every, q_cols), BF16),
            pltpu.VMEM((every, k_cols), BF16),
            pltpu.VMEM((tokens, width), BF16),
            pltpu.VMEM((tokens, width), BF16),
            pltpu.VMEM((every, feats), BF16),
            pltpu.VMEM((feats, q_cols), BF16),
            pltpu.VMEM((feats, k_cols), BF16),
            pltpu.VMEM((tokens, slice_width), BF16),
            pltpu.VMEM((every, feats), BF16),
            pltpu.VMEM((n_row * half, feats), BF16),
            pltpu.VMEM((n_row * half, feats), BF16),
            pltpu.VMEM((n_x, n_row * half, feats), BF16),
            pltpu.VMEM((fold, tokens, feats), BF16),
            pltpu.VMEM((feats, q_cols), BF16),
            pltpu.VMEM((feats, k_cols), BF16),
            pltpu.VMEM((tokens, slice_width), BF16),
            pltpu.VMEM((tokens, 128), F32),
            pltpu.VMEM((1, 128), F32),
            pltpu.VMEM((8, tokens), F32),
            pltpu.VMEM((n_col, 8, tokens), F32),
            pltpu.VMEM((1, slice_width + 128), F32),
            pltpu.VMEM((n_row, 1, slice_width + 128), F32),
            pltpu.VMEM((1, 128), F32),
            pltpu.VMEM((n_col, 1, 128), F32),
            dma((6 + fold,)),
            dma((n_o, 3, 2)),
            dma((n_row, 2)),
            dma((n_row,)),
            dma((n_row,)),
            dma((n_row, n_x)),
            dma((n_row, n_x)),
            dma((n_row, n_x)),
            dma((n_row, n_x)),
            dma((n_row,)),
            dma((n_row,)),
            dma((n_row,)),
            dma((n_x, n_row)),
            dma((n_row,)),
            dma((fold, 2)),
            dma((2, f_tiles)),
            dma((n_col,)),
            dma((n_col,)),
            dma((n_row,)),
            dma((n_row,)),
            dma((n_col,)),
            dma((n_col,)),
        ],
        compiler_params=pltpu.CompilerParams(
            collective_id=0, has_side_effects=True, vmem_limit_bytes=63 * 1024 * 1024
        ),
        name="step",
    )(layer_input, gain.reshape(1, width), d_query, d_keyval, w_query, w_keyval, d_resid)
    return (d_input, grad_wq, grad_wkv, grad_gain.reshape(slice_width), total[0, 0])


def solution(mesh):
    placed = (
        P("row", None),
        P(),
        P("row", "col"),
        P("row", "col"),
        P("row", "col"),
        P("row", "col"),
        P("row", "col"),
    )
    return jax.shard_map(
        local,
        mesh=mesh,
        in_specs=placed,
        out_specs=(P("row", "col"), P("row", "col"), P("row", "col"), P("col"), P()),
        check_vma=False,
    )
```

```python
import functools
import math

import jax
import jax.numpy as jnp
from jax import lax
from jax.experimental import pallas as pl
from jax.experimental.pallas import tpu as pltpu
from jax.sharding import PartitionSpec as P

epsilon = 1e-05
MESH = pl.DeviceIdType.MESH
F32 = jnp.float32
BF16 = jnp.bfloat16
VMEM_LIMIT = 48 * 1024 * 1024


def tile(size, limit):
    return limit if size % limit == 0 else size


def step_kernel(
    n_row, n_col,
    x_hbm, gain_hbm, dq_hbm, dk_hbm, wq_hbm, wk_hbm, resid_hbm,
    dout, gq, gk, gains_out, total_out,
    cotq, cotk, xin, normed, ncols, wq, wk, resid, pfull, precv, csend, xrecv, fg,
    gain, acc_q, acc_k, inv, sq, dots, dots_in, gains, gains_in, tot, tot_in,
    load_sem, cot_send, cot_recv, swap_send, swap_recv, xs_send,
    cs_send, cs_recv, pe_send, pe_recv, xr_send, xr_recv, fs_send, fs_recv,
    dot_send, dot_recv, gain_send, gain_recv, tot_send, tot_recv,
):
    row, col = lax.axis_index("row"), lax.axis_index("col")
    tokens, width = xin.shape
    half = tokens // 2
    feats = width // n_row
    slice_width = width // n_col
    fold = n_row // n_col
    n_o, n_x = n_row // 2, n_col // 2
    o, y = row // 2, row % 2
    x, core = col // 2, col % 2
    mate = row + 1 - 2 * y
    home_col = row // fold
    home_x = home_col // 2
    at_home = x == home_x
    swap_x = (home_x + n_x // 2) % n_x
    halves = fg.shape[1]

    def remote(src, dst, send, recv, to_row, to_col):
        return pltpu.make_async_remote_copy(
            src_ref=src, dst_ref=dst, send_sem=send, recv_sem=recv,
            device_id=(to_row, to_col), device_id_type=MESH,
        )

    barrier = pltpu.get_barrier_semaphore()

    def greet_plane(k, carry):
        r = (row + k // 2) % n_row
        c = 2 * x + (core + k % 2) % 2
        pl.semaphore_signal(barrier, inc=1, device_id=(r, c), device_id_type=MESH)
        return carry

    lax.fori_loop(1, 2 * n_row, greet_plane, 0)

    def greet_cols(k, carry):
        c = (2 * x + k) % n_col
        pl.semaphore_signal(barrier, inc=1, device_id=(row, c), device_id_type=MESH)
        return carry

    lax.fori_loop(2, n_col, greet_cols, 0)
    x_copy = pltpu.make_async_copy(x_hbm, xin, load_sem.at[0])
    x_copy.start()
    gain_copy = pltpu.make_async_copy(gain_hbm, gain, load_sem.at[6])
    gain_copy.start()
    with jax.named_scope("greet"):
        pl.semaphore_wait(barrier, 2 * n_row - 1 + n_col - 2)

    def place(i):
        return (i % 2) * n_o + i // 2

    def block(i):
        return pl.ds(pl.multiple_of(place(i) * tokens, tokens), tokens)

    def nth(j):
        m = jnp.where(o < n_o - 1 - o, o, n_o - 1 - o)
        d = jnp.where(j <= 2 * m, (j + 1) // 2, j - m)
        up = jnp.where(j <= 2 * m, j % 2 == 0, o < n_o - 1 - o)
        return jnp.where(up, o + d, o - d)

    pieces = ((dq_hbm, cotq), (dk_hbm, cotk))

    def cot_copy(way, p, source, to_row, own):
        held = pieces[p][1].at[block(source)]
        return remote(
            pieces[p][0] if own else held, held,
            cot_send.at[source // 2, way, p], cot_recv.at[source, p], to_row, col,
        )

    for p in range(2):
        cot_copy(2, p, row, mate, True).start()

        @pl.when(o + 1 < n_o)
        def _():
            cot_copy(0, p, row, row + 2, True).start()

        @pl.when(o > 0)
        def _():
            cot_copy(1, p, row, row - 2, True).start()

    keep = [
        pltpu.make_async_copy(dq_hbm, cotq.at[block(row)], load_sem.at[1]),
        pltpu.make_async_copy(dk_hbm, cotk.at[block(row)], load_sem.at[2]),
        pltpu.make_async_copy(wq_hbm, wq, load_sem.at[3]),
        pltpu.make_async_copy(wk_hbm, wk, load_sem.at[4]),
    ]
    late = pltpu.make_async_copy(resid_hbm, resid, load_sem.at[5])
    x_copy.wait()
    gain_copy.wait()
    for copy in keep:
        copy.start()
    late.start()

    rows_step = 16

    def norm_rows(i, carry):
        rows = pl.ds(pl.multiple_of(i * rows_step, rows_step), rows_step)
        values = xin[rows, :].astype(F32)
        mean = jnp.sum(values * values, axis=1, keepdims=True) / width
        scale = lax.rsqrt(mean + epsilon)
        inv[rows, :] = jnp.broadcast_to(scale, (rows_step, 128))
        normed[rows, :] = (values * scale * gain[...]).astype(BF16)
        return carry

    with jax.named_scope("norm"):
        lax.fori_loop(0, tokens // rows_step, norm_rows, 0)
    own_cols = pl.ds(pl.multiple_of(row * feats, feats), feats)
    ncols[block(row), :] = normed[:, own_cols]
    for copy in keep:
        copy.wait()

    def rows_of(source, c):
        return ncols.at[pl.ds(pl.multiple_of(place(source) * tokens + c * half, half), half)]

    def swap_plane(source):
        return (source // fold // 2 + n_x // 2) % n_x

    def swap_copy(target):
        src = normed.at[
            pl.ds(pl.multiple_of(core * half, half), half),
            pl.ds(pl.multiple_of(target * feats, feats), feats),
        ]
        return remote(
            src, rows_of(row, core), swap_send.at[target], swap_recv.at[row], target, col
        )

    def x_share(source, i):
        mine = rows_of(source, core)
        to_x = (x + i) % n_x
        return remote(
            mine, mine, xs_send.at[source, i], swap_recv.at[source], row, 2 * to_x + core
        )

    def core_share(source):
        mine = rows_of(source, core)
        return remote(
            mine, mine, cs_send.at[source], cs_recv.at[source], row, 2 * x + 1 - core
        )

    def swap_start(target):
        @pl.when(x == swap_x)
        def _():
            swap_copy(target).start()

    def line_peer(k):
        shift = jnp.where(o < n_o // 2, k, n_o - k)
        return 2 * ((o + shift) % n_o) + y

    def mate_peer(k):
        return 2 * ((o + k) % n_o) + 1 - y

    def take(source):
        mine = rows_of(source, core)
        with jax.named_scope("wait_swap"):
            remote(
                mine, mine, cs_send.at[source], swap_recv.at[source], row, 2 * x + 1 - core
            ).wait_recv()
        core_share(source).start()

    def share_first(source):
        @pl.when(x == swap_plane(source))
        def _():
            take(source)
            for i in range(1, n_x):
                x_share(source, i).start()

    def share_second(source):
        @pl.when(x != swap_plane(source))
        def _():
            take(source)

    def first_shares(peer, start):
        def one(k, carry):
            share_first(peer(k))
            return carry

        lax.fori_loop(start, n_o, one, 0)

    def second_shares(peer, start):
        def one(k, carry):
            share_second(peer(k))
            return carry

        def wait(k, carry):
            core_share(peer(k)).wait_recv()
            return carry

        lax.fori_loop(start, n_o, one, 0)
        with jax.named_scope("wait_share"):
            lax.fori_loop(start, n_o, wait, 0)

    contract = (((1,), (1,)), ((), ()))
    f_tile = tile(feats, 256)
    own_half = pl.multiple_of(core * half, half)
    other_half = pl.multiple_of((1 - core) * half, half)

    def half_rows(source, start):
        return pl.ds(pl.multiple_of(place(source) * tokens + start, half), half)

    def slot(source):
        return pl.ds(pl.multiple_of(source * half, half), half)

    def pair_copy(source, h):
        return remote(
            pfull.at[h, half_rows(source, other_half)], precv.at[h, slot(source)],
            pe_send.at[source, h], pe_recv.at[source, h], row, 2 * x + 1 - core,
        )

    def cross_copy(source, h):
        return remote(
            csend.at[h, slot(source)], xrecv.at[x, h, slot(source)],
            xr_send.at[source, h], xr_recv.at[x, source, h], row, 2 * home_x + core,
        )

    def home_copy(source, h):
        return remote(
            csend.at[h, slot(source)], fg.at[row % fold, h, pl.ds(own_half, half)],
            fs_send.at[source, h], fs_recv.at[row % fold, h, core], source, home_col,
        )

    h_width = feats // halves
    h_tiles = h_width // f_tile

    def stage_one(source, h):
        def one(i, carry):
            fs = pl.ds(pl.multiple_of(h * h_width + i * f_tile, f_tile), f_tile)
            value = lax.dot_general(
                cotq[block(source), :], wq[fs, :], contract, preferred_element_type=F32
            ) + lax.dot_general(
                cotk[block(source), :], wk[fs, :], contract, preferred_element_type=F32
            )
            to = pl.ds(pl.multiple_of(i * f_tile, f_tile), f_tile)
            pfull[h, block(source), to] = value.astype(BF16)
            return carry

        with jax.named_scope("multiply"):
            lax.fori_loop(0, h_tiles, one, 0)
        pair_copy(source, h).start()

    add_rows = tile(half, 32)

    def stage_two(source, h):
        with jax.named_scope("wait_pair"):
            pair_copy(source, h).wait_recv()

        @pl.when(jnp.logical_not(at_home))
        def _():
            def one(i, carry):
                at = i * add_rows
                mine = pl.ds(pl.multiple_of(place(source) * tokens + own_half + at, add_rows), add_rows)
                rows = pl.ds(pl.multiple_of(source * half + at, add_rows), add_rows)
                value = pfull[h, mine, :].astype(F32) + precv[h, rows, :].astype(F32)
                csend[h, rows, :] = value.astype(BF16)
                return carry

            lax.fori_loop(0, half // add_rows, one, 0)
            cross_copy(source, h).start()

    def stage_three(source, h):
        @pl.when(at_home)
        def _():
            for i in range(1, n_x):
                from_x = (x + i) % n_x
                with jax.named_scope("wait_cross"):
                    remote(
                        csend.at[h, slot(source)], xrecv.at[from_x, h, slot(source)],
                        xr_send.at[source, h], xr_recv.at[from_x, source, h],
                        row, 2 * x + 1 - core,
                    ).wait_recv()

            def one(i, carry):
                at = i * add_rows
                mine = pl.ds(pl.multiple_of(place(source) * tokens + own_half + at, add_rows), add_rows)
                rows = pl.ds(pl.multiple_of(source * half + at, add_rows), add_rows)
                value = pfull[h, mine, :].astype(F32) + precv[h, rows, :].astype(F32)
                for k in range(1, n_x):
                    value = value + xrecv[(x + k) % n_x, h, rows, :].astype(F32)
                csend[h, rows, :] = value.astype(BF16)
                return carry

            lax.fori_loop(0, half // add_rows, one, 0)
            here = (source == row) & (home_col == col)

            @pl.when(jnp.logical_not(here))
            def _():
                home_copy(source, h).start()

            @pl.when(here)
            def _():
                fg[row % fold, h, pl.ds(own_half, half), :] = csend[h, slot(source), :]

    down = (((0,), (0,)), ((), ()))
    weight_scale = 1.0 / math.sqrt(tokens)
    groups = []
    for held, kept, total in ((cotq, gq, acc_q), (cotk, gk, acc_k)):
        groups.append((held, kept, total, tile(held.shape[1], 512)))
    line_rows = n_o * tokens

    def products(i, line, action):
        fs = pl.ds(pl.multiple_of(i * f_tile, f_tile), f_tile)
        rows = pl.ds(pl.multiple_of(line * line_rows, line_rows), line_rows)
        for held, kept, total, k_tile in groups:
            for k in range(held.shape[1] // k_tile):
                ks = pl.ds(k * k_tile, k_tile)
                value = lax.dot_general(
                    ncols[rows, fs], held[rows, ks], down, preferred_element_type=F32
                )
                action(value, kept, total, fs, ks, k_tile)

    def line_weights(i, carry):
        def keep_sum(value, kept, total, fs, ks, k_tile):
            total[fs, ks] = value

        products(i, y, keep_sum)
        return carry

    def mate_weights(i, carry):
        def finish(value, kept, total, fs, ks, k_tile):
            value = ((value + total[fs, ks]) * weight_scale).astype(BF16)
            kept[fs, ks] = value
            value = value.astype(F32)
            value = jnp.sum(value * value, axis=0, keepdims=True)
            for at in range(0, k_tile, 128):
                sq[...] += value[:, at : at + 128]

        products(i, 1 - y, finish)
        return carry

    f_tiles = feats // f_tile
    sq[...] = jnp.zeros_like(sq)

    def line_source(j):
        return 2 * nth(j) + y

    def mate_source(j):
        return 2 * nth(j) + 1 - y

    def halves_of(source, action):
        def one(h, carry):
            action(source, h)
            return carry

        lax.fori_loop(0, halves, one, 0)

    def mate_arrival(source):
        for p in range(2):
            with jax.named_scope("wait_mate"):
                cot_copy(0, p, source, mate, False).wait_recv()

    at_end = (o == 0) | (o == n_o - 1)

    def swap_if(target, end):
        line = target // 2

        @pl.when(((line == 0) | (line == n_o - 1)) == end)
        def _():
            swap_start(target)

    def swap_all(peer, start, end):
        def one(k, carry):
            swap_if(peer(k), end)
            return carry

        lax.fori_loop(start, n_o, one, 0)

    def sides(j, action):
        def one(side, carry):
            line = jnp.where(side == 0, o - j, o + j)

            @pl.when((line >= 0) & (line < n_o) & ((j > 0) | (side == 0)))
            def _():
                action(line, side)

            return carry

        lax.fori_loop(0, 2, one, 0)

    def arrive(line, side):
        source = 2 * line + y
        onward = jnp.where(side == 0, o + 1 < n_o, o > 0)
        to_row = jnp.where(side == 0, row + 2, row - 2)
        for p in range(2):
            with jax.named_scope("wait_line"):
                cot_copy(0, p, source, mate, False).wait_recv()

            @pl.when(onward)
            def _():
                cot_copy(0, p, source, to_row, False).start()

            cot_copy(2, p, source, mate, False).start()

    def go_home(line, held):
        late_one = ((line == 0) | (line == n_o - 1)) & jnp.logical_not(at_end)

        @pl.when(late_one == held)
        def _():
            halves_of(2 * line + y, stage_three)

    def main_step(j, carry):
        @pl.when(j >= 1)
        def _():
            sides(j, arrive)
            sides(j - 1, lambda line, side: go_home(line, False))

            @pl.when(at_end)
            def _():
                swap_if(line_peer(j), False)

            @pl.when(jnp.logical_not(at_end) & (j == 2))
            def _():
                swap_all(line_peer, 1, False)

        sides(j, lambda line, side: halves_of(2 * line + y, stage_one))

        @pl.when(j >= 1)
        def _():
            mate_arrival(mate_source(j - 1))
            halves_of(mate_source(j - 1), stage_one)

        sides(j, lambda line, side: halves_of(2 * line + y, stage_two))

        @pl.when(j >= 1)
        def _():
            halves_of(mate_source(j - 1), stage_two)

        return carry

    lax.fori_loop(0, n_o, main_step, 0)
    last = mate_source(n_o - 1)

    def mate_homes(j, carry):
        halves_of(mate_source(j), stage_three)
        return carry

    def held_homes(j, carry):
        go_home(nth(j), True)
        return carry

    def drain_line(j, carry):
        line = nth(j)

        @pl.when(jnp.where(line < o, o + 1 < n_o, o > 0))
        def _():
            for p in range(2):
                cot_copy(0, p, 2 * line + y, mate, False).wait_send()

        return carry

    def drain_mate(j, carry):
        for p in range(2):
            cot_copy(2, p, 2 * nth(j) + y, mate, False).wait_send()
        return carry

    with jax.named_scope("drain_line"):
        for p in range(2):
            @pl.when(o + 1 < n_o)
            def _():
                cot_copy(0, p, row, row + 2, True).wait_send()

            @pl.when(o > 0)
            def _():
                cot_copy(1, p, row, row - 2, True).wait_send()

        lax.fori_loop(1, n_o, drain_line, 0)

    swap_all(line_peer, 1, True)
    lax.fori_loop(0, n_o, held_homes, 0)
    mate_arrival(last)
    with jax.named_scope("drain_mate"):
        for p in range(2):
            cot_copy(2, p, row, mate, True).wait_send()
        lax.fori_loop(1, n_o, drain_mate, 0)
    swap_all(mate_peer, 0, True)
    swap_all(mate_peer, 0, False)
    halves_of(last, stage_one)
    halves_of(last, stage_two)
    sides(n_o - 1, lambda line, side: go_home(line, False))
    first_shares(line_peer, 1)
    lax.fori_loop(0, n_o - 1, mate_homes, 0)
    second_shares(line_peer, 1)
    with jax.named_scope("weights"):
        lax.fori_loop(0, f_tiles, line_weights, 0)
    first_shares(mate_peer, 0)
    halves_of(last, stage_three)
    second_shares(mate_peer, 0)
    with jax.named_scope("weights"):
        lax.fori_loop(0, f_tiles, mate_weights, 0)

    late.wait()
    col_start = col * slice_width
    c_tile = tile(h_width, 256)
    model_width = width
    tiles = h_width // c_tile

    def lanes(value):
        total = value[:, 0:128]
        for k in range(1, c_tile // 128):
            total = total + value[:, k * 128 : (k + 1) * 128]
        return total

    def wide(value):
        return jnp.concatenate([value] * (c_tile // 128), axis=1)

    acc = jnp.zeros((tokens, 128), F32)
    for n in range(fold):
        j = (row + n) % fold
        for h in range(halves):
            for c in range(2):
                @pl.when(jnp.logical_not((col * fold + j == row) & (c == core)))
                def _():
                    arrived = fg.at[j, h, pl.ds(c * half, half)]
                    with jax.named_scope("wait_home"):
                        remote(
                            arrived, arrived, fs_send.at[0, 0], fs_recv.at[j, h, c],
                            row, 2 * x + 1 - core,
                        ).wait_recv()

            for t in range(tiles):
                at = j * feats + h * h_width + t * c_tile
                here = pl.ds(pl.multiple_of(col_start + at, c_tile), c_tile)
                there = pl.ds(pl.multiple_of(at, c_tile), c_tile)
                grad = fg[j, h, :, t * c_tile : (t + 1) * c_tile].astype(F32)
                product = grad * xin[:, here].astype(F32)
                acc = acc + lanes(product * gain[:, here])
                gains[:, there] = jnp.sum(product * wide(inv[...]), axis=0, keepdims=True)
    summed = jnp.broadcast_to(jnp.sum(acc, axis=1, keepdims=True), (tokens, 128))
    dots[...] = jnp.transpose(summed)[0:8, :]
    gains[:, slice_width:] = sq[...]

    dot_copies, gain_copies = [], []
    for k in range(1, n_col):
        dot_copies.append(
            remote(dots, dots_in.at[col], dot_send.at[k], dot_recv.at[k], row, (col + k) % n_col)
        )
    for k in range(1, n_row):
        gain_copies.append(
            remote(gains, gains_in.at[row], gain_send.at[k], gain_recv.at[k], (row + k) % n_row, col)
        )
    for copy in dot_copies + gain_copies:
        copy.start()
    dots_in[col] = dots[...]
    gains_in[row] = gains[...]
    with jax.named_scope("wait_gains"):
        for copy in gain_copies:
            copy.wait()
    all_gains = jnp.sum(gains_in[...], axis=0)
    grad_gain = all_gains[:, :slice_width] * (1.0 / math.sqrt(tokens * n_row))
    gains_out[...] = grad_gain
    squares = jnp.sum(grad_gain * grad_gain) + jnp.sum(all_gains[:, slice_width:])
    tot[...] = jnp.full(tot.shape, squares, F32)
    tot_copies = [
        remote(tot, tot_in.at[col], tot_send.at[k], tot_recv.at[k], row, (col + k) % n_col)
        for k in range(1, n_col)
    ]
    for copy in tot_copies:
        copy.start()
    tot_in[col] = tot[...]
    with jax.named_scope("wait_dots"):
        for copy in dot_copies:
            copy.wait()
    token_row = jnp.sum(dots_in[...], axis=0)[0:1, :]
    token_dot = jnp.transpose(jnp.broadcast_to(token_row, (128, tokens)))
    inv_rms = inv[...]
    inv_wide = wide(inv_rms)
    factor = wide(inv_rms * inv_rms * inv_rms * token_dot / model_width)
    for j in range(fold):
        for h in range(halves):
            for t in range(tiles):
                at = j * feats + h * h_width + t * c_tile
                here = pl.ds(pl.multiple_of(col_start + at, c_tile), c_tile)
                grad = fg[j, h, :, t * c_tile : (t + 1) * c_tile].astype(F32)
                value = (
                    resid[:, at : at + c_tile].astype(F32)
                    + inv_wide * gain[:, here] * grad
                    - xin[:, here].astype(F32) * factor
                )
                dout[:, at : at + c_tile] = value.astype(BF16)
    with jax.named_scope("wait_total"):
        for copy in tot_copies:
            copy.wait()
    total_out[...] = jnp.sum(tot_in[...], axis=0) / model_width

    def drain_row(k, carry):
        source = (row + k) % n_row
        for h in range(halves):
            pair_copy(source, h).wait_send()

            @pl.when(jnp.logical_not(at_home))
            def _():
                cross_copy(source, h).wait_send()

            @pl.when(at_home & jnp.logical_not((source == row) & (home_col == col)))
            def _():
                home_copy(source, h).wait_send()

        @pl.when(k >= 1)
        def _():
            core_share(source).wait_send()

            @pl.when(x == swap_x)
            def _():
                swap_copy(source).wait_send()

            @pl.when(x == swap_plane(source))
            def _():
                for i in range(1, n_x):
                    x_share(source, i).wait_send()

        return carry

    lax.fori_loop(0, n_row, drain_row, 0)


def store_kernel(*refs):
    count = len(refs) // 2
    sems = refs[-1]
    copies = [
        pltpu.make_async_copy(refs[i], refs[count + i], sems.at[i]) for i in range(count)
    ]
    for copy in copies:
        copy.start()
    for copy in copies:
        copy.wait()


def local(layer_input, gain, d_query, d_keyval, w_query, w_keyval, d_resid):
    n_row, n_col = lax.axis_size("row"), lax.axis_size("col")
    n_x, n_o, fold = n_col // 2, n_row // 2, n_row // n_col
    tokens, width = layer_input.shape
    q_cols, k_cols = d_query.shape[1], d_keyval.shape[1]
    feats, slice_width = width // n_row, width // n_col
    half = tokens // 2
    halves = 2 if feats // tile(feats, 256) % 2 == 0 else 1
    h_width = feats // halves
    dma = pltpu.SemaphoreType.DMA
    hbm = pl.BlockSpec(memory_space=pltpu.HBM)
    vmem = pl.BlockSpec(memory_space=pltpu.VMEM)
    shape = jax.ShapeDtypeStruct
    every = n_row * tokens
    pin = functools.partial(pltpu.with_memory_space_constraint, memory_space=pltpu.HBM)
    results = pl.pallas_call(
        functools.partial(step_kernel, n_row, n_col),
        out_shape=(
            pltpu.VMEM((tokens, slice_width), BF16),
            pltpu.VMEM((feats, q_cols), BF16),
            pltpu.VMEM((feats, k_cols), BF16),
            pltpu.VMEM((1, slice_width), F32),
            pltpu.VMEM((1, 128), F32),
        ),
        in_specs=[hbm] * 7,
        out_specs=[vmem] * 5,
        scratch_shapes=[
            pltpu.VMEM((every, q_cols), BF16),
            pltpu.VMEM((every, k_cols), BF16),
            pltpu.VMEM((tokens, width), BF16),
            pltpu.VMEM((tokens, width), BF16),
            pltpu.VMEM((every, feats), BF16),
            pltpu.VMEM((feats, q_cols), BF16),
            pltpu.VMEM((feats, k_cols), BF16),
            pltpu.VMEM((tokens, slice_width), BF16),
            pltpu.VMEM((halves, every, h_width), BF16),
            pltpu.VMEM((halves, n_row * half, h_width), BF16),
            pltpu.VMEM((halves, n_row * half, h_width), BF16),
            pltpu.VMEM((n_x, halves, n_row * half, h_width), BF16),
            pltpu.VMEM((fold, halves, tokens, h_width), BF16),
            pltpu.VMEM((1, width), F32),
            pltpu.VMEM((feats, q_cols), F32),
            pltpu.VMEM((feats, k_cols), F32),
            pltpu.VMEM((tokens, 128), F32),
            pltpu.VMEM((1, 128), F32),
            pltpu.VMEM((8, tokens), F32),
            pltpu.VMEM((n_col, 8, tokens), F32),
            pltpu.VMEM((1, slice_width + 128), F32),
            pltpu.VMEM((n_row, 1, slice_width + 128), F32),
            pltpu.VMEM((1, 128), F32),
            pltpu.VMEM((n_col, 1, 128), F32),
            dma((7,)),
            dma((n_o, 3, 2)),
            dma((n_row, 2)),
            dma((n_row,)),
            dma((n_row,)),
            dma((n_row, n_x)),
            dma((n_row,)),
            dma((n_row,)),
            dma((n_row, halves)),
            dma((n_row, halves)),
            dma((n_row, halves)),
            dma((n_x, n_row, halves)),
            dma((n_row, halves)),
            dma((fold, halves, 2)),
            dma((n_col,)),
            dma((n_col,)),
            dma((n_row,)),
            dma((n_row,)),
            dma((n_col,)),
            dma((n_col,)),
        ],
        compiler_params=pltpu.CompilerParams(
            collective_id=0, has_side_effects=True, vmem_limit_bytes=VMEM_LIMIT
        ),
        name="step",
    )(
        pin(layer_input), pin(gain.reshape(1, width)), pin(d_query), pin(d_keyval),
        pin(w_query), pin(w_keyval), pin(d_resid),
    )
    d_input, grad_wq, grad_wkv, grad_gain, total = pl.pallas_call(
        store_kernel,
        out_shape=tuple(shape(result.shape, result.dtype) for result in results),
        in_specs=[vmem] * 5,
        out_specs=[hbm] * 5,
        scratch_shapes=[dma((5,))],
        compiler_params=pltpu.CompilerParams(vmem_limit_bytes=1024 * 1024),
        name="store",
    )(*results)
    return (d_input, grad_wq, grad_wkv, grad_gain.reshape(slice_width), total[0, 0])


def solution(mesh):
    placed = (
        P("row", None),
        P(),
        P("row", "col"),
        P("row", "col"),
        P("row", "col"),
        P("row", "col"),
        P("row", "col"),
    )
    return jax.shard_map(
        local,
        mesh=mesh,
        in_specs=placed,
        out_specs=(P("row", "col"), P("row", "col"), P("row", "col"), P("col"), P()),
        check_vma=False,
    )
```

```python
import functools
import math

import jax
import jax.numpy as jnp
from jax import lax
from jax.experimental import pallas as pl
from jax.experimental.pallas import tpu as pltpu
from jax.sharding import PartitionSpec as P

epsilon = 1e-05
MESH = pl.DeviceIdType.MESH
F32 = jnp.float32
BF16 = jnp.bfloat16
VMEM_LIMIT = 48 * 1024 * 1024


def tile(size, limit):
    return limit if size % limit == 0 else size


def step_kernel(
    n_row, n_col,
    x_hbm, gain_hbm, dq_hbm, dk_hbm, wq_hbm, wk_hbm, resid_hbm,
    dout, gq, gk, gains_out, total_out,
    cotq, cotk, xin, normed, ncols, wq, wk, resid, pfull, precv, csend, xrecv, fg,
    gain, acc_q, acc_k, inv, sq, dots, dots_in, gains, gains_in, tot, tot_in, sq_in,
    load_sem, cot_send, cot_recv, swap_send, swap_recv, xs_send,
    cs_send, cs_recv, pe_send, pe_recv, xr_send, xr_recv, fs_send, fs_recv,
    dot_send, dot_recv, gain_send, gain_recv, tot_send, tot_recv, sq_send, sq_recv, credit,
):
    row, col = lax.axis_index("row"), lax.axis_index("col")
    tokens, width = xin.shape
    half = tokens // 2
    feats = width // n_row
    slice_width = width // n_col
    fold = n_row // n_col
    n_o, n_x = n_row // 2, n_col // 2
    o, y = row // 2, row % 2
    x, core = col // 2, col % 2
    mate = row + 1 - 2 * y
    home_col = row // fold
    home_x = home_col // 2
    at_home = x == home_x
    swap_x = (home_x + n_x // 2) % n_x
    halves = fg.shape[1]

    def remote(src, dst, send, recv, to_row, to_col):
        return pltpu.make_async_remote_copy(
            src_ref=src, dst_ref=dst, send_sem=send, recv_sem=recv,
            device_id=(to_row, to_col), device_id_type=MESH,
        )

    barrier = pltpu.get_barrier_semaphore()

    def greet_plane(k, carry):
        r = (row + k // 2) % n_row
        c = 2 * x + (core + k % 2) % 2
        pl.semaphore_signal(barrier, inc=1, device_id=(r, c), device_id_type=MESH)
        return carry

    lax.fori_loop(1, 2 * n_row, greet_plane, 0)

    def greet_cols(k, carry):
        c = (2 * x + k) % n_col
        pl.semaphore_signal(barrier, inc=1, device_id=(row, c), device_id_type=MESH)
        return carry

    lax.fori_loop(2, n_col, greet_cols, 0)
    x_copy = pltpu.make_async_copy(x_hbm, xin, load_sem.at[0])
    x_copy.start()
    gain_copy = pltpu.make_async_copy(gain_hbm, gain, load_sem.at[6])
    gain_copy.start()
    with jax.named_scope("greet"):
        pl.semaphore_wait(barrier, 2 * n_row - 1 + n_col - 2)

    def place(i):
        return (i % 2) * n_o + i // 2

    def block(i):
        return pl.ds(pl.multiple_of(place(i) * tokens, tokens), tokens)

    def nth(j):
        m = jnp.where(o < n_o - 1 - o, o, n_o - 1 - o)
        d = jnp.where(j <= 2 * m, (j + 1) // 2, j - m)
        up = jnp.where(j <= 2 * m, j % 2 == 0, o < n_o - 1 - o)
        return jnp.where(up, o + d, o - d)

    pieces = ((dq_hbm, cotq), (dk_hbm, cotk))

    def cot_copy(way, p, source, to_row, own):
        held = pieces[p][1].at[block(source)]
        return remote(
            pieces[p][0] if own else held, held,
            cot_send.at[source // 2, way, p], cot_recv.at[source, p], to_row, col,
        )

    for p in range(2):
        cot_copy(2, p, row, mate, True).start()

        @pl.when(o + 1 < n_o)
        def _():
            cot_copy(0, p, row, row + 2, True).start()

        @pl.when(o > 0)
        def _():
            cot_copy(1, p, row, row - 2, True).start()

    keep = [
        pltpu.make_async_copy(dq_hbm, cotq.at[block(row)], load_sem.at[1]),
        pltpu.make_async_copy(dk_hbm, cotk.at[block(row)], load_sem.at[2]),
        pltpu.make_async_copy(wq_hbm, wq, load_sem.at[3]),
        pltpu.make_async_copy(wk_hbm, wk, load_sem.at[4]),
    ]
    late = pltpu.make_async_copy(resid_hbm, resid, load_sem.at[5])
    x_copy.wait()
    gain_copy.wait()
    for copy in keep:
        copy.start()
    late.start()

    rows_step = 16

    def norm_rows(i, carry):
        rows = pl.ds(pl.multiple_of(i * rows_step, rows_step), rows_step)
        values = xin[rows, :].astype(F32)
        mean = jnp.sum(values * values, axis=1, keepdims=True) / width
        scale = lax.rsqrt(mean + epsilon)
        inv[rows, :] = jnp.broadcast_to(scale, (rows_step, 128))
        normed[rows, :] = (values * scale * gain[...]).astype(BF16)
        return carry

    with jax.named_scope("norm"):
        lax.fori_loop(0, tokens // rows_step, norm_rows, 0)
    own_cols = pl.ds(pl.multiple_of(row * feats, feats), feats)
    ncols[block(row), :] = normed[:, own_cols]
    for copy in keep:
        copy.wait()

    def rows_of(source, c):
        return ncols.at[pl.ds(pl.multiple_of(place(source) * tokens + c * half, half), half)]

    def swap_plane(source):
        return (source // fold // 2 + n_x // 2) % n_x

    def swap_copy(target):
        src = normed.at[
            pl.ds(pl.multiple_of(core * half, half), half),
            pl.ds(pl.multiple_of(target * feats, feats), feats),
        ]
        return remote(
            src, rows_of(row, core), swap_send.at[target], swap_recv.at[row], target, col
        )

    def x_share(source, i):
        mine = rows_of(source, core)
        to_x = (x + i) % n_x
        return remote(
            mine, mine, xs_send.at[source, i], swap_recv.at[source], row, 2 * to_x + core
        )

    def core_share(source):
        mine = rows_of(source, core)
        return remote(
            mine, mine, cs_send.at[source], cs_recv.at[source], row, 2 * x + 1 - core
        )

    def swap_start(target):
        @pl.when(x == swap_x)
        def _():
            swap_copy(target).start()

    def line_peer(k):
        shift = jnp.where(o < n_o // 2, k, n_o - k)
        return 2 * ((o + shift) % n_o) + y

    def mate_peer(k):
        return 2 * ((o + k) % n_o) + 1 - y

    def take(source):
        mine = rows_of(source, core)
        with jax.named_scope("wait_swap"):
            remote(
                mine, mine, cs_send.at[source], swap_recv.at[source], row, 2 * x + 1 - core
            ).wait_recv()
        core_share(source).start()

    def share_first(source):
        @pl.when(x == swap_plane(source))
        def _():
            take(source)
            for i in range(1, n_x):
                x_share(source, i).start()

    def share_second(source):
        @pl.when(x != swap_plane(source))
        def _():
            take(source)

    def first_shares(peer, start):
        def one(k, carry):
            share_first(peer(k))
            return carry

        lax.fori_loop(start, n_o, one, 0)

    def second_shares(peer, start):
        def one(k, carry):
            share_second(peer(k))
            return carry

        lax.fori_loop(start, n_o, one, 0)

    def core_shares(peer, start, direct):
        def wait(k, carry):
            @pl.when((x == swap_plane(peer(k))) == direct)
            def _():
                core_share(peer(k)).wait_recv()

            return carry

        with jax.named_scope("wait_share"):
            lax.fori_loop(start, n_o, wait, 0)

    contract = (((1,), (1,)), ((), ()))
    f_tile = tile(feats, 256)
    own_half = pl.multiple_of(core * half, half)
    other_half = pl.multiple_of((1 - core) * half, half)

    def half_rows(source, start):
        return pl.ds(pl.multiple_of(place(source) * tokens + start, half), half)

    def slot(source):
        return pl.ds(pl.multiple_of(source * half, half), half)

    def pair_copy(source, h):
        return remote(
            pfull.at[h, half_rows(source, other_half)], precv.at[h, slot(source)],
            pe_send.at[source, h], pe_recv.at[source, h], row, 2 * x + 1 - core,
        )

    def cross_copy(source, h):
        return remote(
            csend.at[h, slot(source)], xrecv.at[x, h, slot(source)],
            xr_send.at[source, h], xr_recv.at[x, source, h], row, 2 * home_x + core,
        )

    def home_copy(source, h):
        return remote(
            csend.at[h, slot(source)], fg.at[row % fold, h, pl.ds(own_half, half)],
            fs_send.at[source, h], fs_recv.at[row % fold, h, core], source, home_col,
        )

    h_width = feats // halves
    h_tiles = h_width // f_tile

    def stage_one(source, h):
        def one(i, carry):
            fs = pl.ds(pl.multiple_of(h * h_width + i * f_tile, f_tile), f_tile)
            value = lax.dot_general(
                cotq[block(source), :], wq[fs, :], contract, preferred_element_type=F32
            ) + lax.dot_general(
                cotk[block(source), :], wk[fs, :], contract, preferred_element_type=F32
            )
            to = pl.ds(pl.multiple_of(i * f_tile, f_tile), f_tile)
            pfull[h, block(source), to] = value.astype(BF16)
            return carry

        with jax.named_scope("multiply"):
            lax.fori_loop(0, h_tiles, one, 0)
        pair_copy(source, h).start()

    add_rows = tile(half, 32)

    def stage_two(source, h):
        with jax.named_scope("wait_pair"):
            pair_copy(source, h).wait_recv()

        @pl.when(jnp.logical_not(at_home))
        def _():
            def one(i, carry):
                at = i * add_rows
                mine = pl.ds(pl.multiple_of(place(source) * tokens + own_half + at, add_rows), add_rows)
                rows = pl.ds(pl.multiple_of(source * half + at, add_rows), add_rows)
                value = pfull[h, mine, :].astype(F32) + precv[h, rows, :].astype(F32)
                csend[h, rows, :] = value.astype(BF16)
                return carry

            lax.fori_loop(0, half // add_rows, one, 0)
            cross_copy(source, h).start()

    def stage_three(source, h):
        @pl.when(at_home)
        def _():
            for i in range(1, n_x):
                from_x = (x + i) % n_x
                with jax.named_scope("wait_cross"):
                    remote(
                        csend.at[h, slot(source)], xrecv.at[from_x, h, slot(source)],
                        xr_send.at[source, h], xr_recv.at[from_x, source, h],
                        row, 2 * x + 1 - core,
                    ).wait_recv()

            def one(i, carry):
                at = i * add_rows
                mine = pl.ds(pl.multiple_of(place(source) * tokens + own_half + at, add_rows), add_rows)
                rows = pl.ds(pl.multiple_of(source * half + at, add_rows), add_rows)
                value = pfull[h, mine, :].astype(F32) + precv[h, rows, :].astype(F32)
                for k in range(1, n_x):
                    value = value + xrecv[(x + k) % n_x, h, rows, :].astype(F32)
                csend[h, rows, :] = value.astype(BF16)
                return carry

            lax.fori_loop(0, half // add_rows, one, 0)
            here = (source == row) & (home_col == col)

            @pl.when(jnp.logical_not(here))
            def _():
                home_copy(source, h).start()

            @pl.when(here)
            def _():
                fg[row % fold, h, pl.ds(own_half, half), :] = csend[h, slot(source), :]

    down = (((0,), (0,)), ((), ()))
    weight_scale = 1.0 / math.sqrt(tokens)
    groups = []
    for held, kept, total in ((cotq, gq, acc_q), (cotk, gk, acc_k)):
        groups.append((held, kept, total, tile(held.shape[1], 512)))
    group_lines = n_o // n_x

    def products(i, first, count, action):
        fs = pl.ds(pl.multiple_of(i * f_tile, f_tile), f_tile)
        rows = pl.ds(pl.multiple_of(first * tokens, tokens), count * tokens)
        for held, kept, total, k_tile in groups:
            for k in range(held.shape[1] // k_tile):
                ks = pl.ds(k * k_tile, k_tile)
                value = lax.dot_general(
                    ncols[rows, fs], held[rows, ks], down, preferred_element_type=F32
                )
                action(value, kept, total, fs, ks, k_tile)

    def line_weights(i, carry):
        def keep_sum(value, kept, total, fs, ks, k_tile):
            total[fs, ks] = value

        products(i, y * n_o, n_o, keep_sum)
        return carry

    def mate_weights(group, last_one):
        first = (1 - y) * n_o + group * group_lines

        def one(i, carry):
            def add(value, kept, total, fs, ks, k_tile):
                total[fs, ks] += value

            def finish(value, kept, total, fs, ks, k_tile):
                value = ((value + total[fs, ks]) * weight_scale).astype(BF16)
                kept[fs, ks] = value
                value = value.astype(F32)
                value = jnp.sum(value * value, axis=0, keepdims=True)
                for at in range(0, k_tile, 128):
                    sq[...] += value[:, at : at + 128]

            products(i, first, group_lines, finish if last_one else add)
            return carry

        with jax.named_scope("weights"):
            lax.fori_loop(0, f_tiles, one, 0)

    f_tiles = feats // f_tile
    sq[...] = jnp.zeros_like(sq)

    def line_source(j):
        return 2 * nth(j) + y

    def mate_source(j):
        return 2 * nth(j) + 1 - y

    def halves_of(source, action):
        def one(h, carry):
            action(source, h)
            return carry

        lax.fori_loop(0, halves, one, 0)

    at_end = (o == 0) | (o == n_o - 1)
    inward = jnp.where(o == 0, row + 2, row - 2)
    inward_way = jnp.where(o == 0, 1, 0)

    def by_mate(line):
        low = (o == 1) & (line == 0)
        high = (o == n_o - 2) & (line == n_o - 1)
        return jnp.logical_not(low | high)

    def mate_arrival(source):
        for p in range(2):
            with jax.named_scope("wait_mate"):
                cot_copy(0, p, source, mate, False).wait_recv()

            @pl.when(at_end & (source == mate))
            def _():
                relay_copy(p).start()

    def relay_copy(p):
        held = pieces[p][1].at[block(mate)]
        return remote(
            held, held, cot_send.at[o, inward_way, p], cot_recv.at[mate, p], inward, col
        )

    def swap_if(target, end):
        line = target // 2

        @pl.when(((line == 0) | (line == n_o - 1)) == end)
        def _():
            swap_start(target)

    def swap_all(peer, start, end):
        def one(k, carry):
            swap_if(peer(k), end)
            return carry

        lax.fori_loop(start, n_o, one, 0)

    def sides(j, action):
        def one(side, carry):
            line = jnp.where(side == 0, o - j, o + j)

            @pl.when((line >= 0) & (line < n_o) & ((j > 0) | (side == 0)))
            def _():
                action(line, side)

            return carry

        lax.fori_loop(0, 2, one, 0)

    def arrive(line, side):
        source = 2 * line + y
        onward = jnp.where(side == 0, o + 1 < n_o, o > 0)
        to_row = jnp.where(side == 0, row + 2, row - 2)
        for p in range(2):
            with jax.named_scope("wait_line"):
                cot_copy(0, p, source, mate, False).wait_recv()

            @pl.when(onward)
            def _():
                cot_copy(0, p, source, to_row, False).start()

            @pl.when(by_mate(line))
            def _():
                cot_copy(2, p, source, mate, False).start()

    def go_home(line, held):
        late_one = ((line == 0) | (line == n_o - 1)) & jnp.logical_not(at_end)

        @pl.when(late_one == held)
        def _():
            halves_of(2 * line + y, stage_three)

    def main_step(j, carry):
        @pl.when(j >= 1)
        def _():
            sides(j, arrive)
            sides(j - 1, lambda line, side: go_home(line, False))

            @pl.when(at_end)
            def _():
                swap_if(line_peer(j), False)

            @pl.when(jnp.logical_not(at_end) & (j == 2))
            def _():
                swap_all(line_peer, 1, False)

        sides(j, lambda line, side: halves_of(2 * line + y, stage_one))

        @pl.when(j >= 1)
        def _():
            mate_arrival(mate_source(j - 1))
            halves_of(mate_source(j - 1), stage_one)

        sides(j, lambda line, side: halves_of(2 * line + y, stage_two))

        @pl.when(j >= 1)
        def _():
            halves_of(mate_source(j - 1), stage_two)

        return carry

    lax.fori_loop(0, n_o, main_step, 0)
    last = mate_source(n_o - 1)

    def mate_homes(j, carry):
        halves_of(mate_source(j), stage_three)
        return carry

    def held_homes(j, carry):
        go_home(nth(j), True)
        return carry

    def drain_line(j, carry):
        line = nth(j)

        @pl.when(jnp.where(line < o, o + 1 < n_o, o > 0))
        def _():
            for p in range(2):
                cot_copy(0, p, 2 * line + y, mate, False).wait_send()

        return carry

    def drain_mate(j, carry):
        @pl.when(by_mate(nth(j)))
        def _():
            for p in range(2):
                cot_copy(2, p, 2 * nth(j) + y, mate, False).wait_send()

        return carry

    with jax.named_scope("drain_line"):
        for p in range(2):
            @pl.when(o + 1 < n_o)
            def _():
                cot_copy(0, p, row, row + 2, True).wait_send()

            @pl.when(o > 0)
            def _():
                cot_copy(1, p, row, row - 2, True).wait_send()

        lax.fori_loop(1, n_o, drain_line, 0)

        @pl.when(at_end)
        def _():
            for p in range(2):
                relay_copy(p).wait_send()

    own_end = jnp.where(o == 0, 0, 1)

    def tell(peer, start, base):
        def one(k, carry):
            pl.semaphore_signal(
                credit.at[base + own_end], inc=1,
                device_id=(peer(k), col), device_id_type=MESH,
            )
            return carry

        @pl.when(at_end)
        def _():
            lax.fori_loop(start, n_o, one, 0)

    def heed(base):
        for i in range(2):
            @pl.when((base == 2) | (o != i * (n_o - 1)))
            def _():
                pl.semaphore_wait(credit.at[base + i], 1)

    tell(line_peer, 1, 0)

    @pl.when(at_end)
    def _():
        swap_all(mate_peer, 0, False)

    mate_arrival(last)
    tell(mate_peer, 0, 2)
    with jax.named_scope("drain_mate"):
        for p in range(2):
            cot_copy(2, p, row, mate, True).wait_send()
        lax.fori_loop(1, n_o, drain_mate, 0)

    @pl.when(jnp.logical_not(at_end))
    def _():
        swap_all(mate_peer, 0, False)

    halves_of(last, stage_one)
    halves_of(last, stage_two)
    with jax.named_scope("heed_line"):
        heed(0)
    swap_all(line_peer, 1, True)
    lax.fori_loop(0, n_o, held_homes, 0)
    sides(n_o - 1, lambda line, side: go_home(line, False))
    with jax.named_scope("heed_mate"):
        heed(2)
    swap_all(mate_peer, 0, True)
    first_shares(line_peer, 1)
    lax.fori_loop(0, n_o - 1, mate_homes, 0)
    halves_of(last, stage_three)
    second_shares(line_peer, 1)
    first_shares(mate_peer, 0)
    core_shares(line_peer, 1, True)
    core_shares(line_peer, 1, False)
    with jax.named_scope("weights"):
        lax.fori_loop(0, f_tiles, line_weights, 0)
    core_shares(mate_peer, 0, True)
    mate_weights((x + n_x // 2) % n_x, n_x == 1)
    second_shares(mate_peer, 0)
    core_shares(mate_peer, 0, False)

    late.wait()
    col_start = col * slice_width
    c_tile = tile(h_width, 256)
    model_width = width
    tiles = h_width // c_tile

    def lanes(value):
        total = value[:, 0:128]
        for k in range(1, c_tile // 128):
            total = total + value[:, k * 128 : (k + 1) * 128]
        return total

    def wide(value):
        return jnp.concatenate([value] * (c_tile // 128), axis=1)

    acc = jnp.zeros((tokens, 128), F32)
    for n in range(fold):
        j = (row + n) % fold
        for h in range(halves):
            for c in range(2):
                @pl.when(jnp.logical_not((col * fold + j == row) & (c == core)))
                def _():
                    arrived = fg.at[j, h, pl.ds(c * half, half)]
                    with jax.named_scope("wait_home"):
                        remote(
                            arrived, arrived, fs_send.at[0, 0], fs_recv.at[j, h, c],
                            row, 2 * x + 1 - core,
                        ).wait_recv()

            for t in range(tiles):
                at = j * feats + h * h_width + t * c_tile
                here = pl.ds(pl.multiple_of(col_start + at, c_tile), c_tile)
                there = pl.ds(pl.multiple_of(at, c_tile), c_tile)
                grad = fg[j, h, :, t * c_tile : (t + 1) * c_tile].astype(F32)
                product = grad * xin[:, here].astype(F32)
                acc = acc + lanes(product * gain[:, here])
                gains[:, there] = jnp.sum(product * wide(inv[...]), axis=0, keepdims=True)
    summed = jnp.broadcast_to(jnp.sum(acc, axis=1, keepdims=True), (tokens, 128))
    dots[...] = jnp.transpose(summed)[0:8, :]

    dot_copies, gain_copies = [], []
    for k in range(1, n_col):
        dot_copies.append(
            remote(dots, dots_in.at[col], dot_send.at[k], dot_recv.at[k], row, (col + k) % n_col)
        )
    for k in range(1, n_row):
        gain_copies.append(
            remote(gains, gains_in.at[row], gain_send.at[k], gain_recv.at[k], (row + k) % n_row, col)
        )
    for copy in dot_copies + gain_copies:
        copy.start()
    for i in range(1, n_x):
        mate_weights((x + n_x // 2 + i) % n_x, i == n_x - 1)
    square_copies = [
        remote(sq, sq_in.at[row], sq_send.at[k], sq_recv.at[k], (row + k) % n_row, col)
        for k in range(1, n_row)
    ]
    for copy in square_copies:
        copy.start()
    sq_in[row] = sq[...]
    dots_in[col] = dots[...]
    gains_in[row] = gains[...]
    with jax.named_scope("wait_gains"):
        for copy in gain_copies:
            copy.wait()
    grad_gain = jnp.sum(gains_in[...], axis=0) * (1.0 / math.sqrt(tokens * n_row))
    gains_out[...] = grad_gain
    gain_squares = jnp.sum(grad_gain * grad_gain)
    with jax.named_scope("wait_squares"):
        for copy in square_copies:
            copy.wait()
    tot[...] = jnp.full(tot.shape, gain_squares + jnp.sum(sq_in[...]), F32)
    tot_copies = [
        remote(tot, tot_in.at[col], tot_send.at[k], tot_recv.at[k], row, (col + k) % n_col)
        for k in range(1, n_col)
    ]
    for copy in tot_copies:
        copy.start()
    tot_in[col] = tot[...]
    with jax.named_scope("wait_dots"):
        for copy in dot_copies:
            copy.wait()
    token_row = jnp.sum(dots_in[...], axis=0)[0:1, :]
    token_dot = jnp.transpose(jnp.broadcast_to(token_row, (128, tokens)))
    inv_rms = inv[...]
    inv_wide = wide(inv_rms)
    factor = wide(inv_rms * inv_rms * inv_rms * token_dot / model_width)
    for j in range(fold):
        for h in range(halves):
            for t in range(tiles):
                at = j * feats + h * h_width + t * c_tile
                here = pl.ds(pl.multiple_of(col_start + at, c_tile), c_tile)
                grad = fg[j, h, :, t * c_tile : (t + 1) * c_tile].astype(F32)
                value = (
                    resid[:, at : at + c_tile].astype(F32)
                    + inv_wide * gain[:, here] * grad
                    - xin[:, here].astype(F32) * factor
                )
                dout[:, at : at + c_tile] = value.astype(BF16)
    with jax.named_scope("wait_total"):
        for copy in tot_copies:
            copy.wait()
    total_out[...] = jnp.sum(tot_in[...], axis=0) / model_width

    def drain_row(k, carry):
        source = (row + k) % n_row
        for h in range(halves):
            pair_copy(source, h).wait_send()

            @pl.when(jnp.logical_not(at_home))
            def _():
                cross_copy(source, h).wait_send()

            @pl.when(at_home & jnp.logical_not((source == row) & (home_col == col)))
            def _():
                home_copy(source, h).wait_send()

        @pl.when(k >= 1)
        def _():
            core_share(source).wait_send()

            @pl.when(x == swap_x)
            def _():
                swap_copy(source).wait_send()

            @pl.when(x == swap_plane(source))
            def _():
                for i in range(1, n_x):
                    x_share(source, i).wait_send()

        return carry

    lax.fori_loop(0, n_row, drain_row, 0)


def store_kernel(*refs):
    count = len(refs) // 2
    sems = refs[-1]
    copies = [
        pltpu.make_async_copy(refs[i], refs[count + i], sems.at[i]) for i in range(count)
    ]
    for copy in copies:
        copy.start()
    for copy in copies:
        copy.wait()


def local(layer_input, gain, d_query, d_keyval, w_query, w_keyval, d_resid):
    n_row, n_col = lax.axis_size("row"), lax.axis_size("col")
    n_x, n_o, fold = n_col // 2, n_row // 2, n_row // n_col
    tokens, width = layer_input.shape
    q_cols, k_cols = d_query.shape[1], d_keyval.shape[1]
    feats, slice_width = width // n_row, width // n_col
    half = tokens // 2
    halves = 2 if feats // tile(feats, 256) % 2 == 0 else 1
    h_width = feats // halves
    dma = pltpu.SemaphoreType.DMA
    hbm = pl.BlockSpec(memory_space=pltpu.HBM)
    vmem = pl.BlockSpec(memory_space=pltpu.VMEM)
    shape = jax.ShapeDtypeStruct
    every = n_row * tokens
    pin = functools.partial(pltpu.with_memory_space_constraint, memory_space=pltpu.HBM)
    results = pl.pallas_call(
        functools.partial(step_kernel, n_row, n_col),
        out_shape=(
            pltpu.VMEM((tokens, slice_width), BF16),
            pltpu.VMEM((feats, q_cols), BF16),
            pltpu.VMEM((feats, k_cols), BF16),
            pltpu.VMEM((1, slice_width), F32),
            pltpu.VMEM((1, 128), F32),
        ),
        in_specs=[hbm] * 7,
        out_specs=[vmem] * 5,
        scratch_shapes=[
            pltpu.VMEM((every, q_cols), BF16),
            pltpu.VMEM((every, k_cols), BF16),
            pltpu.VMEM((tokens, width), BF16),
            pltpu.VMEM((tokens, width), BF16),
            pltpu.VMEM((every, feats), BF16),
            pltpu.VMEM((feats, q_cols), BF16),
            pltpu.VMEM((feats, k_cols), BF16),
            pltpu.VMEM((tokens, slice_width), BF16),
            pltpu.VMEM((halves, every, h_width), BF16),
            pltpu.VMEM((halves, n_row * half, h_width), BF16),
            pltpu.VMEM((halves, n_row * half, h_width), BF16),
            pltpu.VMEM((n_x, halves, n_row * half, h_width), BF16),
            pltpu.VMEM((fold, halves, tokens, h_width), BF16),
            pltpu.VMEM((1, width), F32),
            pltpu.VMEM((feats, q_cols), F32),
            pltpu.VMEM((feats, k_cols), F32),
            pltpu.VMEM((tokens, 128), F32),
            pltpu.VMEM((1, 128), F32),
            pltpu.VMEM((8, tokens), F32),
            pltpu.VMEM((n_col, 8, tokens), F32),
            pltpu.VMEM((1, slice_width), F32),
            pltpu.VMEM((n_row, 1, slice_width), F32),
            pltpu.VMEM((1, 128), F32),
            pltpu.VMEM((n_col, 1, 128), F32),
            pltpu.VMEM((n_row, 1, 128), F32),
            dma((7,)),
            dma((n_o, 3, 2)),
            dma((n_row, 2)),
            dma((n_row,)),
            dma((n_row,)),
            dma((n_row, n_x)),
            dma((n_row,)),
            dma((n_row,)),
            dma((n_row, halves)),
            dma((n_row, halves)),
            dma((n_row, halves)),
            dma((n_x, n_row, halves)),
            dma((n_row, halves)),
            dma((fold, halves, 2)),
            dma((n_col,)),
            dma((n_col,)),
            dma((n_row,)),
            dma((n_row,)),
            dma((n_col,)),
            dma((n_col,)),
            dma((n_row,)),
            dma((n_row,)),
            pltpu.SemaphoreType.REGULAR((4,)),
        ],
        compiler_params=pltpu.CompilerParams(
            collective_id=0, has_side_effects=True, vmem_limit_bytes=VMEM_LIMIT
        ),
        name="step",
    )(
        pin(layer_input), pin(gain.reshape(1, width)), pin(d_query), pin(d_keyval),
        pin(w_query), pin(w_keyval), pin(d_resid),
    )
    d_input, grad_wq, grad_wkv, grad_gain, total = pl.pallas_call(
        store_kernel,
        out_shape=tuple(shape(result.shape, result.dtype) for result in results),
        in_specs=[vmem] * 5,
        out_specs=[hbm] * 5,
        scratch_shapes=[dma((5,))],
        compiler_params=pltpu.CompilerParams(vmem_limit_bytes=1024 * 1024),
        name="store",
    )(*results)
    return (d_input, grad_wq, grad_wkv, grad_gain.reshape(slice_width), total[0, 0])


def solution(mesh):
    placed = (
        P("row", None),
        P(),
        P("row", "col"),
        P("row", "col"),
        P("row", "col"),
        P("row", "col"),
        P("row", "col"),
    )
    return jax.shard_map(
        local,
        mesh=mesh,
        in_specs=placed,
        out_specs=(P("row", "col"), P("row", "col"), P("row", "col"), P("col"), P()),
        check_vma=False,
    )
```

```python
import functools
import math

import jax
import jax.numpy as jnp
from jax import lax
from jax.experimental import pallas as pl
from jax.experimental.pallas import tpu as pltpu
from jax.sharding import PartitionSpec as P

epsilon = 1e-05
MESH = pl.DeviceIdType.MESH
F32 = jnp.float32
BF16 = jnp.bfloat16
VMEM_LIMIT = 48 * 1024 * 1024


def tile(size, limit):
    return limit if size % limit == 0 else size


def step_kernel(
    n_row, n_col,
    x_hbm, gain_hbm, dq_hbm, dk_hbm, wq_hbm, wk_hbm, resid_hbm,
    dout, gq, gk, gains_out, total_out,
    cotq, cotk, xin, normed, ncols, wq, wk, resid, pfull, precv, csend, xrecv, fg,
    gain, acc_q, acc_k, inv, sq, dots, dots_in, gains, gains_in, tot, tot_in, sq_in,
    load_sem, cot_send, cot_recv, swap_send, swap_recv, xs_send,
    cs_send, cs_recv, pe_send, pe_recv, xr_send, xr_recv, fs_send, fs_recv,
    dot_send, dot_recv, gain_send, gain_recv, tot_send, tot_recv, sq_send, sq_recv, credit,
):
    row, col = lax.axis_index("row"), lax.axis_index("col")
    tokens, width = xin.shape
    half = tokens // 2
    feats = width // n_row
    slice_width = width // n_col
    fold = n_row // n_col
    n_o, n_x = n_row // 2, n_col // 2
    o, y = row // 2, row % 2
    x, core = col // 2, col % 2
    mate = row + 1 - 2 * y
    home_col = row // fold
    home_x = home_col // 2
    at_home = x == home_x
    swap_x = (home_x + n_x // 2) % n_x
    halves = fg.shape[1]

    def remote(src, dst, send, recv, to_row, to_col):
        return pltpu.make_async_remote_copy(
            src_ref=src, dst_ref=dst, send_sem=send, recv_sem=recv,
            device_id=(to_row, to_col), device_id_type=MESH,
        )

    barrier = pltpu.get_barrier_semaphore()

    def greet_plane(k, carry):
        r = (row + k // 2) % n_row
        c = 2 * x + (core + k % 2) % 2
        pl.semaphore_signal(barrier, inc=1, device_id=(r, c), device_id_type=MESH)
        return carry

    lax.fori_loop(1, 2 * n_row, greet_plane, 0)

    def greet_cols(k, carry):
        c = (2 * x + k) % n_col
        pl.semaphore_signal(barrier, inc=1, device_id=(row, c), device_id_type=MESH)
        return carry

    lax.fori_loop(2, n_col, greet_cols, 0)
    x_copy = pltpu.make_async_copy(x_hbm, xin, load_sem.at[0])
    x_copy.start()
    gain_copy = pltpu.make_async_copy(gain_hbm, gain, load_sem.at[6])
    gain_copy.start()
    with jax.named_scope("greet"):
        pl.semaphore_wait(barrier, 2 * n_row - 1 + n_col - 2)

    def place(i):
        return (i % 2) * n_o + i // 2

    def block(i):
        return pl.ds(pl.multiple_of(place(i) * tokens, tokens), tokens)

    def nth(j):
        m = jnp.where(o < n_o - 1 - o, o, n_o - 1 - o)
        d = jnp.where(j <= 2 * m, (j + 1) // 2, j - m)
        up = jnp.where(j <= 2 * m, j % 2 == 0, o < n_o - 1 - o)
        return jnp.where(up, o + d, o - d)

    pieces = ((dq_hbm, cotq), (dk_hbm, cotk))

    def cot_copy(way, p, source, to_row, own):
        held = pieces[p][1].at[block(source)]
        return remote(
            pieces[p][0] if own else held, held,
            cot_send.at[source // 2, way, p], cot_recv.at[source, p], to_row, col,
        )

    for p in range(2):
        cot_copy(2, p, row, mate, True).start()

        @pl.when(o + 1 < n_o)
        def _():
            cot_copy(0, p, row, row + 2, True).start()

        @pl.when(o > 0)
        def _():
            cot_copy(1, p, row, row - 2, True).start()

    keep = [
        pltpu.make_async_copy(dq_hbm, cotq.at[block(row)], load_sem.at[1]),
        pltpu.make_async_copy(dk_hbm, cotk.at[block(row)], load_sem.at[2]),
        pltpu.make_async_copy(wq_hbm, wq, load_sem.at[3]),
        pltpu.make_async_copy(wk_hbm, wk, load_sem.at[4]),
    ]
    late = pltpu.make_async_copy(resid_hbm, resid, load_sem.at[5])
    x_copy.wait()
    gain_copy.wait()
    for copy in keep:
        copy.start()
    late.start()

    rows_step = 16

    def norm_rows(i, carry):
        rows = pl.ds(pl.multiple_of(i * rows_step, rows_step), rows_step)
        values = xin[rows, :].astype(F32)
        mean = jnp.sum(values * values, axis=1, keepdims=True) / width
        scale = lax.rsqrt(mean + epsilon)
        inv[rows, :] = jnp.broadcast_to(scale, (rows_step, 128))
        normed[rows, :] = (values * scale * gain[...]).astype(BF16)
        return carry

    with jax.named_scope("norm"):
        lax.fori_loop(0, tokens // rows_step, norm_rows, 0)
    own_cols = pl.ds(pl.multiple_of(row * feats, feats), feats)
    ncols[block(row), :] = normed[:, own_cols]
    for copy in keep:
        copy.wait()

    def rows_of(source, c):
        return ncols.at[pl.ds(pl.multiple_of(place(source) * tokens + c * half, half), half)]

    def swap_plane(source):
        return (source // fold // 2 + n_x // 2) % n_x

    def swap_copy(target):
        src = normed.at[
            pl.ds(pl.multiple_of(core * half, half), half),
            pl.ds(pl.multiple_of(target * feats, feats), feats),
        ]
        return remote(
            src, rows_of(row, core), swap_send.at[target], swap_recv.at[row], target, col
        )

    def x_share(source, i):
        mine = rows_of(source, core)
        to_x = (x + i) % n_x
        return remote(
            mine, mine, xs_send.at[source, i], swap_recv.at[source], row, 2 * to_x + core
        )

    def core_share(source):
        mine = rows_of(source, core)
        return remote(
            mine, mine, cs_send.at[source], cs_recv.at[source], row, 2 * x + 1 - core
        )

    def swap_start(target):
        @pl.when(x == swap_x)
        def _():
            swap_copy(target).start()

    def line_peer(k):
        shift = jnp.where(o < n_o // 2, k, n_o - k)
        return 2 * ((o + shift) % n_o) + y

    def mate_peer(k):
        return 2 * ((o + k) % n_o) + 1 - y

    def take(source):
        mine = rows_of(source, core)
        with jax.named_scope("wait_swap"):
            remote(
                mine, mine, cs_send.at[source], swap_recv.at[source], row, 2 * x + 1 - core
            ).wait_recv()
        core_share(source).start()

    def share_first(source):
        @pl.when(x == swap_plane(source))
        def _():
            take(source)
            for i in range(1, n_x):
                x_share(source, i).start()

    def share_second(source):
        @pl.when(x != swap_plane(source))
        def _():
            take(source)

    def first_shares(peer, start):
        def one(k, carry):
            share_first(peer(k))
            return carry

        lax.fori_loop(start, n_o, one, 0)

    def second_shares(peer, start):
        def one(k, carry):
            share_second(peer(k))
            return carry

        lax.fori_loop(start, n_o, one, 0)

    def core_shares(peer, start, direct):
        def wait(k, carry):
            @pl.when((x == swap_plane(peer(k))) == direct)
            def _():
                core_share(peer(k)).wait_recv()

            return carry

        with jax.named_scope("wait_share"):
            lax.fori_loop(start, n_o, wait, 0)

    contract = (((1,), (1,)), ((), ()))
    f_tile = tile(feats, 256)
    own_half = pl.multiple_of(core * half, half)
    other_half = pl.multiple_of((1 - core) * half, half)

    def half_rows(source, start):
        return pl.ds(pl.multiple_of(place(source) * tokens + start, half), half)

    def slot(source):
        return pl.ds(pl.multiple_of(source * half, half), half)

    def pair_copy(source, h):
        return remote(
            pfull.at[h, half_rows(source, other_half)], precv.at[h, slot(source)],
            pe_send.at[source, h], pe_recv.at[source, h], row, 2 * x + 1 - core,
        )

    def cross_copy(source, h):
        return remote(
            csend.at[h, slot(source)], xrecv.at[x, h, slot(source)],
            xr_send.at[source, h], xr_recv.at[x, source, h], row, 2 * home_x + core,
        )

    def home_copy(source, h):
        return remote(
            csend.at[h, slot(source)], fg.at[row % fold, h, pl.ds(own_half, half)],
            fs_send.at[source, h], fs_recv.at[row % fold, h, core], source, home_col,
        )

    h_width = feats // halves
    h_tiles = h_width // f_tile

    def stage_one(source, h):
        def one(i, carry):
            fs = pl.ds(pl.multiple_of(h * h_width + i * f_tile, f_tile), f_tile)
            value = lax.dot_general(
                cotq[block(source), :], wq[fs, :], contract, preferred_element_type=F32
            ) + lax.dot_general(
                cotk[block(source), :], wk[fs, :], contract, preferred_element_type=F32
            )
            to = pl.ds(pl.multiple_of(i * f_tile, f_tile), f_tile)
            pfull[h, block(source), to] = value.astype(BF16)
            return carry

        with jax.named_scope("multiply"):
            lax.fori_loop(0, h_tiles, one, 0)
        pair_copy(source, h).start()

    add_rows = tile(half, 32)

    def stage_two(source, h):
        with jax.named_scope("wait_pair"):
            pair_copy(source, h).wait_recv()

        @pl.when(jnp.logical_not(at_home))
        def _():
            def one(i, carry):
                at = i * add_rows
                mine = pl.ds(pl.multiple_of(place(source) * tokens + own_half + at, add_rows), add_rows)
                rows = pl.ds(pl.multiple_of(source * half + at, add_rows), add_rows)
                value = pfull[h, mine, :].astype(F32) + precv[h, rows, :].astype(F32)
                csend[h, rows, :] = value.astype(BF16)
                return carry

            lax.fori_loop(0, half // add_rows, one, 0)
            cross_copy(source, h).start()

    def stage_three(source, h):
        @pl.when(at_home)
        def _():
            for i in range(1, n_x):
                from_x = (x + i) % n_x
                with jax.named_scope("wait_cross"):
                    remote(
                        csend.at[h, slot(source)], xrecv.at[from_x, h, slot(source)],
                        xr_send.at[source, h], xr_recv.at[from_x, source, h],
                        row, 2 * x + 1 - core,
                    ).wait_recv()

            def one(i, carry):
                at = i * add_rows
                mine = pl.ds(pl.multiple_of(place(source) * tokens + own_half + at, add_rows), add_rows)
                rows = pl.ds(pl.multiple_of(source * half + at, add_rows), add_rows)
                value = pfull[h, mine, :].astype(F32) + precv[h, rows, :].astype(F32)
                for k in range(1, n_x):
                    value = value + xrecv[(x + k) % n_x, h, rows, :].astype(F32)
                csend[h, rows, :] = value.astype(BF16)
                return carry

            lax.fori_loop(0, half // add_rows, one, 0)
            here = (source == row) & (home_col == col)

            @pl.when(jnp.logical_not(here))
            def _():
                home_copy(source, h).start()

            @pl.when(here)
            def _():
                fg[row % fold, h, pl.ds(own_half, half), :] = csend[h, slot(source), :]

    down = (((0,), (0,)), ((), ()))
    weight_scale = 1.0 / math.sqrt(tokens)
    groups = []
    for held, kept, total in ((cotq, gq, acc_q), (cotk, gk, acc_k)):
        groups.append((held, kept, total, tile(held.shape[1], 512)))
    group_lines = n_o // n_x

    def products(i, first, count, action):
        fs = pl.ds(pl.multiple_of(i * f_tile, f_tile), f_tile)
        rows = pl.ds(pl.multiple_of(first * tokens, tokens), count * tokens)
        for held, kept, total, k_tile in groups:
            for k in range(held.shape[1] // k_tile):
                ks = pl.ds(k * k_tile, k_tile)
                value = lax.dot_general(
                    ncols[rows, fs], held[rows, ks], down, preferred_element_type=F32
                )
                action(value, kept, total, fs, ks, k_tile)

    def line_weights(i, carry):
        def keep_sum(value, kept, total, fs, ks, k_tile):
            total[fs, ks] = value

        products(i, y * n_o, n_o, keep_sum)
        return carry

    def mate_weights(group, last_one):
        first = (1 - y) * n_o + group * group_lines

        def one(i, carry):
            def add(value, kept, total, fs, ks, k_tile):
                total[fs, ks] += value

            def finish(value, kept, total, fs, ks, k_tile):
                value = ((value + total[fs, ks]) * weight_scale).astype(BF16)
                kept[fs, ks] = value
                value = value.astype(F32)
                value = jnp.sum(value * value, axis=0, keepdims=True)
                for at in range(0, k_tile, 128):
                    sq[...] += value[:, at : at + 128]

            products(i, first, group_lines, finish if last_one else add)
            return carry

        with jax.named_scope("weights"):
            lax.fori_loop(0, f_tiles, one, 0)

    f_tiles = feats // f_tile
    sq[...] = jnp.zeros_like(sq)

    def line_source(j):
        return 2 * nth(j) + y

    def mate_source(j):
        return 2 * nth(j) + 1 - y

    def halves_of(source, action):
        def one(h, carry):
            action(source, h)
            return carry

        lax.fori_loop(0, halves, one, 0)

    at_end = (o == 0) | (o == n_o - 1)
    inward = jnp.where(o == 0, row + 2, row - 2)
    inward_way = jnp.where(o == 0, 1, 0)

    def by_mate(line):
        low = (o == 1) & (line == 0)
        high = (o == n_o - 2) & (line == n_o - 1)
        return jnp.logical_not(low | high)

    def mate_arrival(source):
        for p in range(2):
            with jax.named_scope("wait_mate"):
                cot_copy(0, p, source, mate, False).wait_recv()

            @pl.when(at_end & (source == mate))
            def _():
                relay_copy(p).start()

    def relay_copy(p):
        held = pieces[p][1].at[block(mate)]
        return remote(
            held, held, cot_send.at[o, inward_way, p], cot_recv.at[mate, p], inward, col
        )

    def swap_if(target, end):
        line = target // 2

        @pl.when(((line == 0) | (line == n_o - 1)) == end)
        def _():
            swap_start(target)

    def swap_all(peer, start, end):
        def one(k, carry):
            swap_if(peer(k), end)
            return carry

        lax.fori_loop(start, n_o, one, 0)

    def sides(j, action):
        def one(side, carry):
            line = jnp.where(side == 0, o - j, o + j)

            @pl.when((line >= 0) & (line < n_o) & ((j > 0) | (side == 0)))
            def _():
                action(line, side)

            return carry

        lax.fori_loop(0, 2, one, 0)

    def arrive(line, side):
        source = 2 * line + y
        onward = jnp.where(side == 0, o + 1 < n_o, o > 0)
        to_row = jnp.where(side == 0, row + 2, row - 2)
        for p in range(2):
            with jax.named_scope("wait_line"):
                cot_copy(0, p, source, mate, False).wait_recv()

            @pl.when(onward)
            def _():
                cot_copy(0, p, source, to_row, False).start()

            @pl.when(by_mate(line))
            def _():
                cot_copy(2, p, source, mate, False).start()

    def go_home(line, held):
        late_one = ((line == 0) | (line == n_o - 1)) & jnp.logical_not(at_end)

        @pl.when(late_one == held)
        def _():
            halves_of(2 * line + y, stage_three)

    def main_step(j, carry):
        @pl.when(j >= 1)
        def _():
            sides(j, arrive)
            sides(j - 1, lambda line, side: go_home(line, False))

            @pl.when(at_end)
            def _():
                swap_if(line_peer(j), False)

            @pl.when(jnp.logical_not(at_end) & (j == 2))
            def _():
                swap_all(line_peer, 1, False)

        sides(j, lambda line, side: halves_of(2 * line + y, stage_one))

        @pl.when(j >= 1)
        def _():
            mate_arrival(mate_source(j - 1))
            halves_of(mate_source(j - 1), stage_one)

        sides(j, lambda line, side: halves_of(2 * line + y, stage_two))

        @pl.when(j >= 1)
        def _():
            halves_of(mate_source(j - 1), stage_two)

        return carry

    lax.fori_loop(0, n_o, main_step, 0)
    last = mate_source(n_o - 1)

    def mate_homes(j, carry):
        halves_of(mate_source(j), stage_three)
        return carry

    def held_homes(j, carry):
        go_home(nth(j), True)
        return carry

    def drain_line(j, carry):
        line = nth(j)

        @pl.when(jnp.where(line < o, o + 1 < n_o, o > 0))
        def _():
            for p in range(2):
                cot_copy(0, p, 2 * line + y, mate, False).wait_send()

        return carry

    def drain_mate(j, carry):
        @pl.when(by_mate(nth(j)))
        def _():
            for p in range(2):
                cot_copy(2, p, 2 * nth(j) + y, mate, False).wait_send()

        return carry

    with jax.named_scope("drain_line"):
        for p in range(2):
            @pl.when(o + 1 < n_o)
            def _():
                cot_copy(0, p, row, row + 2, True).wait_send()

            @pl.when(o > 0)
            def _():
                cot_copy(1, p, row, row - 2, True).wait_send()

        lax.fori_loop(1, n_o, drain_line, 0)

        @pl.when(at_end)
        def _():
            for p in range(2):
                relay_copy(p).wait_send()

    own_end = jnp.where(o == 0, 0, 1)

    def tell(peer, start, base):
        def one(k, carry):
            pl.semaphore_signal(
                credit.at[base + own_end], inc=1,
                device_id=(peer(k), col), device_id_type=MESH,
            )
            return carry

        @pl.when(at_end)
        def _():
            lax.fori_loop(start, n_o, one, 0)

    def heed(base):
        for i in range(2):
            @pl.when((base == 2) | (o != i * (n_o - 1)))
            def _():
                pl.semaphore_wait(credit.at[base + i], 1)

    tell(line_peer, 1, 0)

    @pl.when(at_end)
    def _():
        swap_all(mate_peer, 0, False)

    mate_arrival(last)
    tell(mate_peer, 0, 2)
    with jax.named_scope("drain_mate"):
        for p in range(2):
            cot_copy(2, p, row, mate, True).wait_send()
        lax.fori_loop(1, n_o, drain_mate, 0)

    @pl.when(jnp.logical_not(at_end))
    def _():
        swap_all(mate_peer, 0, False)

    halves_of(last, stage_one)
    halves_of(last, stage_two)
    with jax.named_scope("heed_line"):
        heed(0)
    swap_all(line_peer, 1, True)
    lax.fori_loop(0, n_o, held_homes, 0)
    sides(n_o - 1, lambda line, side: go_home(line, False))
    with jax.named_scope("heed_mate"):
        heed(2)
    swap_all(mate_peer, 0, True)
    first_shares(line_peer, 1)
    lax.fori_loop(0, n_o - 1, mate_homes, 0)
    halves_of(last, stage_three)
    second_shares(line_peer, 1)
    first_shares(mate_peer, 0)
    core_shares(line_peer, 1, True)
    core_shares(line_peer, 1, False)
    with jax.named_scope("weights"):
        lax.fori_loop(0, f_tiles, line_weights, 0)
    core_shares(mate_peer, 0, True)
    mate_weights((x + n_x // 2) % n_x, n_x == 1)
    second_shares(mate_peer, 0)
    core_shares(mate_peer, 0, False)

    late.wait()
    col_start = col * slice_width
    c_tile = tile(h_width, 256)
    model_width = width
    tiles = h_width // c_tile

    def lanes(value):
        total = value[:, 0:128]
        for k in range(1, c_tile // 128):
            total = total + value[:, k * 128 : (k + 1) * 128]
        return total

    def wide(value):
        return jnp.concatenate([value] * (c_tile // 128), axis=1)

    acc = jnp.zeros((tokens, 128), F32)
    for n in range(fold):
        j = (row + n) % fold
        for h in range(halves):
            for c in range(2):
                @pl.when(jnp.logical_not((col * fold + j == row) & (c == core)))
                def _():
                    arrived = fg.at[j, h, pl.ds(c * half, half)]
                    with jax.named_scope("wait_home"):
                        remote(
                            arrived, arrived, fs_send.at[0, 0], fs_recv.at[j, h, c],
                            row, 2 * x + 1 - core,
                        ).wait_recv()

            for t in range(tiles):
                at = j * feats + h * h_width + t * c_tile
                here = pl.ds(pl.multiple_of(col_start + at, c_tile), c_tile)
                there = pl.ds(pl.multiple_of(at, c_tile), c_tile)
                grad = fg[j, h, :, t * c_tile : (t + 1) * c_tile].astype(F32)
                product = grad * xin[:, here].astype(F32)
                acc = acc + lanes(product * gain[:, here])
                gains[:, there] = jnp.sum(product * wide(inv[...]), axis=0, keepdims=True)
    summed = jnp.broadcast_to(jnp.sum(acc, axis=1, keepdims=True), (tokens, 128))
    dots[...] = jnp.transpose(summed)[0:8, :]

    dot_copies, gain_copies = [], []
    for k in range(1, n_col):
        dot_copies.append(
            remote(dots, dots_in.at[col], dot_send.at[k], dot_recv.at[k], row, (col + k) % n_col)
        )
    for k in range(1, n_row):
        gain_copies.append(
            remote(gains, gains_in.at[row], gain_send.at[k], gain_recv.at[k], (row + k) % n_row, col)
        )
    for copy in dot_copies + gain_copies:
        copy.start()
    for i in range(1, n_x):
        mate_weights((x + n_x // 2 + i) % n_x, i == n_x - 1)
    square_copies = [
        remote(sq, sq_in.at[row], sq_send.at[k], sq_recv.at[k], (row + k) % n_row, col)
        for k in range(1, n_row)
    ]
    for copy in square_copies:
        copy.start()
    sq_in[row] = sq[...]
    dots_in[col] = dots[...]
    gains_in[row] = gains[...]
    def drain_row(k, carry):
        source = (row + k) % n_row
        for h in range(halves):
            pair_copy(source, h).wait_send()

            @pl.when(jnp.logical_not(at_home))
            def _():
                cross_copy(source, h).wait_send()

            @pl.when(at_home & jnp.logical_not((source == row) & (home_col == col)))
            def _():
                home_copy(source, h).wait_send()

        @pl.when(k >= 1)
        def _():
            core_share(source).wait_send()

            @pl.when(x == swap_x)
            def _():
                swap_copy(source).wait_send()

            @pl.when(x == swap_plane(source))
            def _():
                for i in range(1, n_x):
                    x_share(source, i).wait_send()

        return carry

    lax.fori_loop(0, n_row, drain_row, 0)

    with jax.named_scope("wait_gains"):
        for copy in gain_copies:
            copy.wait()
    grad_gain = jnp.sum(gains_in[...], axis=0) * (1.0 / math.sqrt(tokens * n_row))
    gains_out[...] = grad_gain
    gain_squares = jnp.sum(grad_gain * grad_gain)
    with jax.named_scope("wait_squares"):
        for copy in square_copies:
            copy.wait()
    tot[...] = jnp.full(tot.shape, gain_squares + jnp.sum(sq_in[...]), F32)
    tot_copies = [
        remote(tot, tot_in.at[col], tot_send.at[k], tot_recv.at[k], row, (col + k) % n_col)
        for k in range(1, n_col)
    ]
    for copy in tot_copies:
        copy.start()
    tot_in[col] = tot[...]
    with jax.named_scope("wait_dots"):
        for copy in dot_copies:
            copy.wait()
    token_row = jnp.sum(dots_in[...], axis=0)[0:1, :]
    token_dot = jnp.transpose(jnp.broadcast_to(token_row, (128, tokens)))
    inv_rms = inv[...]
    inv_wide = wide(inv_rms)
    factor = wide(inv_rms * inv_rms * inv_rms * token_dot / model_width)
    for j in range(fold):
        for h in range(halves):
            for t in range(tiles):
                at = j * feats + h * h_width + t * c_tile
                here = pl.ds(pl.multiple_of(col_start + at, c_tile), c_tile)
                grad = fg[j, h, :, t * c_tile : (t + 1) * c_tile].astype(F32)
                value = (
                    resid[:, at : at + c_tile].astype(F32)
                    + inv_wide * gain[:, here] * grad
                    - xin[:, here].astype(F32) * factor
                )
                dout[:, at : at + c_tile] = value.astype(BF16)
    with jax.named_scope("wait_total"):
        for copy in tot_copies:
            copy.wait()
    total_out[...] = jnp.sum(tot_in[...], axis=0) / model_width


def store_kernel(*refs):
    count = len(refs) // 2
    sems = refs[-1]
    copies = [
        pltpu.make_async_copy(refs[i], refs[count + i], sems.at[i]) for i in range(count)
    ]
    for copy in copies:
        copy.start()
    for copy in copies:
        copy.wait()


def local(layer_input, gain, d_query, d_keyval, w_query, w_keyval, d_resid):
    n_row, n_col = lax.axis_size("row"), lax.axis_size("col")
    n_x, n_o, fold = n_col // 2, n_row // 2, n_row // n_col
    tokens, width = layer_input.shape
    q_cols, k_cols = d_query.shape[1], d_keyval.shape[1]
    feats, slice_width = width // n_row, width // n_col
    half = tokens // 2
    halves = 2 if feats // tile(feats, 256) % 2 == 0 else 1
    h_width = feats // halves
    dma = pltpu.SemaphoreType.DMA
    hbm = pl.BlockSpec(memory_space=pltpu.HBM)
    vmem = pl.BlockSpec(memory_space=pltpu.VMEM)
    shape = jax.ShapeDtypeStruct
    every = n_row * tokens
    pin = functools.partial(pltpu.with_memory_space_constraint, memory_space=pltpu.HBM)
    results = pl.pallas_call(
        functools.partial(step_kernel, n_row, n_col),
        out_shape=(
            pltpu.VMEM((tokens, slice_width), BF16),
            pltpu.VMEM((feats, q_cols), BF16),
            pltpu.VMEM((feats, k_cols), BF16),
            pltpu.VMEM((1, slice_width), F32),
            pltpu.VMEM((1, 128), F32),
        ),
        in_specs=[hbm] * 7,
        out_specs=[vmem] * 5,
        scratch_shapes=[
            pltpu.VMEM((every, q_cols), BF16),
            pltpu.VMEM((every, k_cols), BF16),
            pltpu.VMEM((tokens, width), BF16),
            pltpu.VMEM((tokens, width), BF16),
            pltpu.VMEM((every, feats), BF16),
            pltpu.VMEM((feats, q_cols), BF16),
            pltpu.VMEM((feats, k_cols), BF16),
            pltpu.VMEM((tokens, slice_width), BF16),
            pltpu.VMEM((halves, every, h_width), BF16),
            pltpu.VMEM((halves, n_row * half, h_width), BF16),
            pltpu.VMEM((halves, n_row * half, h_width), BF16),
            pltpu.VMEM((n_x, halves, n_row * half, h_width), BF16),
            pltpu.VMEM((fold, halves, tokens, h_width), BF16),
            pltpu.VMEM((1, width), F32),
            pltpu.VMEM((feats, q_cols), F32),
            pltpu.VMEM((feats, k_cols), F32),
            pltpu.VMEM((tokens, 128), F32),
            pltpu.VMEM((1, 128), F32),
            pltpu.VMEM((8, tokens), F32),
            pltpu.VMEM((n_col, 8, tokens), F32),
            pltpu.VMEM((1, slice_width), F32),
            pltpu.VMEM((n_row, 1, slice_width), F32),
            pltpu.VMEM((1, 128), F32),
            pltpu.VMEM((n_col, 1, 128), F32),
            pltpu.VMEM((n_row, 1, 128), F32),
            dma((7,)),
            dma((n_o, 3, 2)),
            dma((n_row, 2)),
            dma((n_row,)),
            dma((n_row,)),
            dma((n_row, n_x)),
            dma((n_row,)),
            dma((n_row,)),
            dma((n_row, halves)),
            dma((n_row, halves)),
            dma((n_row, halves)),
            dma((n_x, n_row, halves)),
            dma((n_row, halves)),
            dma((fold, halves, 2)),
            dma((n_col,)),
            dma((n_col,)),
            dma((n_row,)),
            dma((n_row,)),
            dma((n_col,)),
            dma((n_col,)),
            dma((n_row,)),
            dma((n_row,)),
            pltpu.SemaphoreType.REGULAR((4,)),
        ],
        compiler_params=pltpu.CompilerParams(
            collective_id=0, has_side_effects=True, vmem_limit_bytes=VMEM_LIMIT
        ),
        name="step",
    )(
        pin(layer_input), pin(gain.reshape(1, width)), pin(d_query), pin(d_keyval),
        pin(w_query), pin(w_keyval), pin(d_resid),
    )
    d_input, grad_wq, grad_wkv, grad_gain, total = pl.pallas_call(
        store_kernel,
        out_shape=tuple(shape(result.shape, result.dtype) for result in results),
        in_specs=[vmem] * 5,
        out_specs=[hbm] * 5,
        scratch_shapes=[dma((5,))],
        compiler_params=pltpu.CompilerParams(vmem_limit_bytes=1024 * 1024),
        name="store",
    )(*results)
    return (d_input, grad_wq, grad_wkv, grad_gain.reshape(slice_width), total[0, 0])


def solution(mesh):
    placed = (
        P("row", None),
        P(),
        P("row", "col"),
        P("row", "col"),
        P("row", "col"),
        P("row", "col"),
        P("row", "col"),
    )
    return jax.shard_map(
        local,
        mesh=mesh,
        in_specs=placed,
        out_specs=(P("row", "col"), P("row", "col"), P("row", "col"), P("col"), P()),
        check_vma=False,
    )
```
